32 devices in a mesh: band: 8 (over z, y), grid: 4 (over x, core).
Axes of the slice: x: 2, y: 2, z: 4, core: 2. Of those that a mesh axis runs over, the one named last changes fastest.
Arguments:
- bands: bfloat16 [2, 16, 128, 128, 128], P(None, 'band', 'grid'), may hold values from -6 to 6
- occupations: float32 [16], P('band'), may hold values from 0.25 to 1
- external: float32 [128, 128, 128], P('grid'), may hold values from 0 to 2
- density_in: float32 [128, 128, 128], P('grid'), may hold values from -0.2 to 1.4
- prev_density: float32 [128, 128, 128], P('grid'), may hold values from 0 to 1.2
- prev_residual: float32 [128, 128, 128], P('grid'), may hold values from -1.3 to 0.3
- hist_density: float32 [5, 128, 128, 128], P(None, 'grid'), may hold values from 0 to 1
- hist_residual: float32 [5, 128, 128, 128], P(None, 'grid'), may hold values from -0.6 to 1
Outputs:
- density: float32 [128, 128, 128], P('grid')
- residual: float32 [128, 128, 128], P('grid')
The draws below stay inside these ranges and needn't reach their ends.
All inputs are finite; a program needn't handle non-finite values.
Results may differ from the reference program's by a relative error of at most 0.018.
The reference program's roundings to bfloat16 on the way count: a program that leaves them out, or rounds other values in their place, can miss the bound.
Values may be sent and summed in bfloat16 or wider, within the bound.
A program may use at most 192 MiB of HBM per device.

```python
import math
import jax
import jax.numpy as jnp
from jax import lax

NG = 128
DEPTH = 6
ITERS = 3
BANDS = 16


def draw_density_in(key, part):
    jitter = jax.random.uniform(key, (NG, NG, NG), jnp.float32, -0.4, 0.4)
    position = jnp.arange(NG, dtype=jnp.float32)[:, None, None] / (NG - 1)
    return 0.2 + 0.8 * position + jitter


def draw_prev_residual(key, part):
    jitter = jax.random.uniform(jax.random.fold_in(key, 11), (NG, NG, NG), jnp.float32, -0.3, 0.3)
    position = jnp.arange(NG, dtype=jnp.float32)[:, None, None] / (NG - 1)
    return -(0.2 + 0.8 * position) + jitter


def draw_hist_residual(key, part):
    jitter = jax.random.uniform(jax.random.fold_in(key, 23), (DEPTH - 1, NG, NG, NG), jnp.float32, -0.3, 0.3)
    position = jnp.arange(NG, dtype=jnp.float32) / (NG - 1)
    order = DEPTH - 1 - jnp.arange(DEPTH - 1, dtype=jnp.float32)
    profile = 0.2 + 0.5 * jnp.cos(math.pi * order[:, None] * position[None, :])
    return profile[:, :, None, None] + jitter


def level_of(rng, shape, cuts, least, largest):
    level = 1.0
    for axis_at, parts in cuts:
        draws = jax.random.uniform(jax.random.fold_in(jax.random.fold_in(rng, 6), axis_at), (parts,), jnp.float32, least / len(cuts), largest / len(cuts))
        level = level * jnp.repeat(jnp.exp(draws), shape[axis_at] // parts).reshape((-1,) + (1,) * (len(shape) - 1 - axis_at))
    return level


def scatter_about(key, shape, spread, reach, shards=(), held_as=jnp.bfloat16):
    entries = jax.random.normal(key, shape, jnp.float32) * spread
    if len(shards) > 0:
        entries = level_of(key, shape, shards, -0.22, 0.18) * entries
    return jnp.clip(entries, min=-reach, max=reach).astype(held_as)


def setup_inputs(seed: int = 0) -> dict:
    streams_of = jax.random.split(jax.random.key(seed), 9)
    bands = scatter_about(streams_of[0], (2, BANDS, NG, NG, NG), 1.0, 6.0, ((1, 8), (2, 4)))
    occupations = jnp.clip(jnp.exp(math.log(1.0) - 1.3862944 * jax.random.uniform(streams_of[1], (BANDS,), jnp.float32) ** level_of(streams_of[1], (BANDS,), ((0, 8),), -0.2, 0.2)), 0.25, 1.0)
    external = jnp.clip(2.0 * jax.random.uniform(streams_of[2], (NG, NG, NG), jnp.float32) ** level_of(streams_of[2], (NG, NG, NG), ((0, 4),), -0.2, 0.2), 0.0, 2.0)
    density_in = draw_density_in(jax.random.fold_in(streams_of[8], 71), 0)
    prev_density = jnp.clip(1.2 * jax.random.uniform(streams_of[4], (NG, NG, NG), jnp.float32) ** level_of(streams_of[4], (NG, NG, NG), ((0, 4),), -0.2, 0.2), 0.0, 1.2)
    prev_residual = draw_prev_residual(jax.random.fold_in(streams_of[8], 71), 0)
    hist_density = jnp.clip(1.0 * jax.random.uniform(streams_of[6], (DEPTH - 1, NG, NG, NG), jnp.float32) ** level_of(streams_of[6], (DEPTH - 1, NG, NG, NG), ((1, 4),), -0.2, 0.2), 0.0, 1.0)
    hist_residual = draw_hist_residual(jax.random.fold_in(streams_of[8], 71), 0)
    return dict(bands=bands, occupations=occupations, external=external, density_in=density_in, prev_density=prev_density, prev_residual=prev_residual, hist_density=hist_density, hist_residual=hist_residual)


time_step = 0.25
energy_shift = 2.5
coupling = 1.0
mixing_weight = 0.5
ridge_share = 0.1
ridge_floor = 0.01
density_scale = 8.0
highest = lax.Precision.HIGHEST

def fourier_tables(length, frequency):
    positions = jnp.arange(length, dtype=jnp.int32)
    phase_index = positions[:, None] * frequency[None, :] % length
    angles = phase_index.astype(jnp.float32) * (2.0 * math.pi / length)
    unit_scale = 1.0 / math.sqrt(length)
    return ((jnp.cos(angles) * unit_scale).astype(jnp.bfloat16), (jnp.sin(angles) * unit_scale).astype(jnp.bfloat16))

def solve_definite(matrix, vector):
    extent = matrix.shape[0]
    factor_low = jnp.zeros_like(matrix)
    for column in range(extent):
        pivot_value = jnp.sqrt(matrix[column, column] - jnp.sum(factor_low[column, :column] * factor_low[column, :column]))
        factor_low = factor_low.at[column, column].set(pivot_value)
        for row_index in range(column + 1, extent):
            element = (matrix[row_index, column] - jnp.sum(factor_low[row_index, :column] * factor_low[column, :column])) / pivot_value
            factor_low = factor_low.at[row_index, column].set(element)
    middle = jnp.zeros_like(vector)
    for row_index in range(extent):
        element = (vector[row_index] - jnp.sum(factor_low[row_index, :row_index] * middle[:row_index])) / factor_low[row_index, row_index]
        middle = middle.at[row_index].set(element)
    result = jnp.zeros_like(vector)
    for row_index in reversed(range(extent)):
        element = (middle[row_index] - jnp.sum(factor_low[row_index + 1:, row_index] * result[row_index + 1:])) / factor_low[row_index, row_index]
        result = result.at[row_index].set(element)
    return result

def contract(operand, matrix):
    return jnp.einsum('abl,lk->abk', operand, matrix, precision=highest)

def along_axis(real_part, imag_part, cosine_part, sine_part, orientation, axis_index):
    cosine_wide = cosine_part.astype(jnp.float32)
    sine_wide = sine_part.astype(jnp.float32) * orientation
    real_moved = jnp.moveaxis(real_part.astype(jnp.float32), axis_index, -1)
    imag_moved = jnp.moveaxis(imag_part.astype(jnp.float32), axis_index, -1)
    out_real = contract(real_moved, cosine_wide) - contract(imag_moved, sine_wide)
    out_imag = contract(real_moved, sine_wide) + contract(imag_moved, cosine_wide)
    return (jnp.moveaxis(out_real, -1, axis_index), jnp.moveaxis(out_imag, -1, axis_index))

def band_step(real_part, imag_part, factor, kinetic, tables):
    cosine_part, sine_part = tables
    real_part = (real_part.astype(jnp.float32) * factor).astype(jnp.bfloat16)
    imag_part = (imag_part.astype(jnp.float32) * factor).astype(jnp.bfloat16)
    for axis_index in (2, 1):
        real_part, imag_part = along_axis(real_part, imag_part, cosine_part, sine_part, -1.0, axis_index)
        real_part = real_part.astype(jnp.bfloat16)
        imag_part = imag_part.astype(jnp.bfloat16)
    real_part, imag_part = along_axis(real_part, imag_part, cosine_part, sine_part, -1.0, 0)
    real_part = (real_part * kinetic).astype(jnp.bfloat16)
    imag_part = (imag_part * kinetic).astype(jnp.bfloat16)
    for axis_index in (0, 1, 2):
        real_part, imag_part = along_axis(real_part, imag_part, cosine_part.T, sine_part.T, 1.0, axis_index)
        real_part = real_part.astype(jnp.bfloat16)
        imag_part = imag_part.astype(jnp.bfloat16)
    return (real_part, imag_part)

def reference(bands, occupations, external, density_in, prev_density, prev_residual, hist_density, hist_residual):
    frequency = jnp.arange(-(NG // 4), NG // 4, dtype=jnp.int32)
    tables = fourier_tables(NG, frequency)
    squared = frequency.astype(jnp.float32) * frequency.astype(jnp.float32)
    quarter = NG / 4.0
    radius = squared[:, None, None] + squared[None, :, None] + squared[None, None, :]
    kinetic = jnp.exp(-time_step * radius / (quarter * quarter))
    cells_total = NG * NG * NG
    real_bands = bands[0]
    imag_bands = bands[1]
    density_now = density_in
    density_prev = prev_density
    residual_prev = prev_residual
    density_diffs = hist_density
    residual_diffs = hist_residual
    residual = density_in
    for iteration in range(ITERS):
        factor = jnp.exp(-time_step * (external + coupling * density_now - energy_shift))

        def one_band(accumulated, slices):
            real_part, imag_part, weight = slices
            real_part, imag_part = band_step(real_part, imag_part, factor, kinetic, tables)
            wide_real = real_part.astype(jnp.float32)
            wide_imag = imag_part.astype(jnp.float32)
            return (accumulated + weight * (wide_real * wide_real + wide_imag * wide_imag), (real_part, imag_part))
        accumulated, (real_bands, imag_bands) = lax.scan(one_band, jnp.zeros((NG, NG, NG), jnp.float32), (real_bands, imag_bands, occupations))
        density_out = accumulated * (density_scale / BANDS)
        residual = density_out - density_now
        density_diffs = jnp.concatenate([density_diffs[density_diffs.shape[0] - (DEPTH - 1):], (density_now - density_prev)[None]], axis=0)
        residual_diffs = jnp.concatenate([residual_diffs[residual_diffs.shape[0] - (DEPTH - 1):], (residual - residual_prev)[None]], axis=0)
        flat_diffs = residual_diffs.reshape(DEPTH, -1)
        gram_matrix = jnp.dot(flat_diffs, flat_diffs.T, precision=highest) / cells_total
        right_side = jnp.dot(flat_diffs, residual.reshape(-1), precision=highest) / cells_total
        ridge_value = ridge_share * jnp.trace(gram_matrix) / DEPTH + ridge_floor
        coeffs = solve_definite(gram_matrix + ridge_value * jnp.eye(DEPTH, dtype=jnp.float32), right_side)
        combined = density_diffs + mixing_weight * residual_diffs
        density_next = density_now + mixing_weight * residual - jnp.einsum('j,jxyz->xyz', coeffs, combined, precision=highest)
        density_prev = density_now
        residual_prev = residual
        density_now = density_next
    return (density_now, residual)
```

```python
import functools
import math

import jax
import jax.numpy as jnp
import numpy as np
from jax import lax
from jax.experimental import pallas as pl
from jax.experimental.pallas import tpu as pltpu
from jax.sharding import PartitionSpec as P

DEPTH = 6
ITERS = 3

time_step = 0.25
energy_shift = 2.5
coupling = 1.0
mixing_weight = 0.5
ridge_share = 0.1
ridge_floor = 0.01
density_scale = 8.0

MESH = pl.DeviceIdType.MESH
BF = jnp.bfloat16
F32 = jnp.float32


def make_tables(ng):
    freq = np.arange(-(ng // 4), ng // 4)
    phase = (np.arange(ng)[:, None] * freq[None, :]) % ng
    angles = phase.astype(np.float64) * (2.0 * math.pi / ng)
    cos = (np.cos(angles) / math.sqrt(ng)).astype(np.float32)
    sin = (np.sin(angles) / math.sqrt(ng)).astype(np.float32)
    forward_z = np.concatenate(
        [np.concatenate([cos, -sin, -sin, -cos], 1), np.concatenate([sin, cos, cos, -sin], 1)], 0
    )
    forward = np.concatenate([cos.T, sin.T], 1)
    inverse = np.concatenate([cos, -sin], 1)
    inverse_z = np.concatenate(
        [np.concatenate([cos.T, sin.T], 1), np.concatenate([-sin.T, cos.T], 1)], 0
    )
    quarter = ng / 4.0
    damp = np.exp(-time_step * (freq.astype(np.float64) ** 2) / (quarter * quarter))
    damp = damp * ((freq >= -(ng // 4)) & (freq < ng // 4))
    pair = damp[:, None] * np.concatenate([damp, damp])[None, :]
    single = np.broadcast_to(damp[:, None], (damp.shape[0], 2 * damp.shape[0]))
    as_bf = lambda table: jnp.asarray(table, F32).astype(BF)
    return (
        as_bf(forward_z),
        as_bf(forward),
        as_bf(inverse),
        as_bf(inverse_z),
        jnp.asarray(pair, F32),
        jnp.asarray(np.ascontiguousarray(single), F32),
    )


def dot(a, b):
    return jnp.dot(a, b, preferred_element_type=F32)


def fold(cells):
    return jnp.sum(cells.reshape(-1, 8, cells.shape[-1]), axis=0)


def spot(j, k):
    return (j * (j + 1) // 2 + k) if j >= k else (k * (k + 1) // 2 + j)


def solve(gram, vector):
    trace = gram[0, 0]
    for j in range(1, DEPTH):
        trace = trace + gram[j, j]
    ridge = trace * (ridge_share / DEPTH) + ridge_floor
    matrix = {(j, k): gram[j, k] + ridge if j == k else gram[j, k] for (j, k) in gram}
    vector = list(vector)
    inverse = []
    for k in range(DEPTH):
        inverse.append(1.0 / matrix[k, k])
        scaled = {j: matrix[j, k] * inverse[k] for j in range(k + 1, DEPTH)}
        for j in range(k + 1, DEPTH):
            vector[j] = vector[j] - scaled[j] * vector[k]
            for m in range(k + 1, j + 1):
                matrix[j, m] = matrix[j, m] - scaled[j] * matrix[m, k]
    for k in reversed(range(DEPTH)):
        value = vector[k]
        for j in range(k + 1, DEPTH):
            value = value - matrix[j, k] * vector[j]
        vector[k] = value * inverse[k]
    return vector


def kernel(
    dims,
    occ_in,
    bands,
    external,
    density_in,
    prev_density,
    prev_residual,
    hist_density,
    hist_residual,
    fz,
    fy,
    iy,
    iz,
    pair_damp,
    single_damp,
    density_out,
    residual_out,
    psi,
    send_f,
    recv_f,
    send_b,
    recv_b,
    xscr,
    dscr,
    fac,
    ext,
    rho0,
    q_hist,
    t_hist,
    now,
    res,
    prev,
    parts,
    sums,
    gsc,
    occ,
    gath,
    staged,
    load_sem,
    f1_send,
    f1_recv,
    f_send,
    f_recv,
    b_send,
    b_recv,
    e_send,
    e_recv,
    a_send,
    a_recv,
    o_send,
    o_recv,
    g_send,
    g_recv,
    out_sem,
):
    G, M, H, NB, PL, C, K, PB, NG = dims
    kept = C * G
    peers = G * M
    xs = C + 8
    ds = NG + 8
    g = lax.axis_index("grid")
    b = lax.axis_index("band")
    m = lax.rem(b, M)
    h = b // M
    rank = m * G + g

    def place(r):
        other = lax.rem(rank + r, peers)
        return other // G, lax.rem(other, G)

    def source(r):
        other = lax.rem(rank + peers - r, peers)
        return other // G, lax.rem(other, G)

    def device(mm, gg):
        return (h * M + mm, gg)

    loads = []

    def load(src, dst):
        copy = pltpu.make_async_copy(src, dst, load_sem.at[len(loads)])
        copy.start()
        loads.append(copy)
        return copy

    first = [load(external, ext), load(density_in, rho0)]
    for t in range(NB):
        for j in range(M):
            for c in range(2):
                first.append(load(bands.at[c, t, pl.ds(j * PL, PL)], psi.at[t, j, c]))
    mine = pl.ds(m * PL, PL)
    later = [
        load(density_in.at[mine], now.at[0]),
        load(prev_density.at[mine], prev),
        load(prev_residual.at[mine], res.at[0]),
    ]
    for j in range(DEPTH - 1):
        later.append(load(hist_residual.at[j, mine], q_hist.at[j]))
        later.append(load(hist_density.at[j, mine], t_hist.at[j]))

    barrier = pltpu.get_barrier_semaphore()

    def greet(r, _):
        mm, gg = place(r)
        pl.semaphore_signal(barrier, inc=1, device_id=device(mm, gg), device_id_type=MESH)
        return 0

    lax.fori_loop(1, peers, greet, 0)

    def greet_half(r, _):
        hh = lax.rem(h + r, H)
        pl.semaphore_signal(barrier, inc=1, device_id=(hh * M + m, g), device_id_type=MESH)
        return 0

    lax.fori_loop(1, H, greet_half, 0)

    lane = lax.broadcasted_iota(jnp.int32, (1, NG), 1)
    sign = jnp.where(lane < NG // 2, 1.0, -1.0).astype(F32)

    def rot(x):
        return pltpu.roll(x, NG // 2, 1) * sign

    def f1_copy(t, r):
        gg = lax.rem(g + r, G)
        return pltpu.make_async_remote_copy(
            src_ref=send_f.at[t, gg],
            dst_ref=recv_f.at[t, g],
            send_sem=f1_send.at[t, r],
            recv_sem=f1_recv.at[t, r],
            device_id=(b, gg),
            device_id_type=MESH,
        )

    def f_copy(t, r):
        mm, gg = place(r)
        return pltpu.make_async_remote_copy(
            src_ref=send_f.at[t, gg, mm],
            dst_ref=recv_f.at[t, g, m],
            send_sem=f_send.at[t, r],
            recv_sem=f_recv.at[t, r],
            device_id=device(mm, gg),
            device_id_type=MESH,
        )

    def b_copy(k, r):
        mm, gg = place(r)
        return pltpu.make_async_remote_copy(
            src_ref=send_b.at[k, gg, mm],
            dst_ref=recv_b.at[k, m, g],
            send_sem=b_send.at[k, r],
            recv_sem=b_recv.at[k, r],
            device_id=device(mm, gg),
            device_id_type=MESH,
        )

    def e_copy(it, k, r):
        hh = lax.rem(h + r, H)
        rows = pl.ds(k * PB, PB)
        return pltpu.make_async_remote_copy(
            src_ref=parts.at[it, h, rows],
            dst_ref=parts.at[it, h, rows],
            send_sem=e_send.at[it, k, r],
            recv_sem=e_recv.at[it, k, r],
            device_id=(hh * M + m, g),
            device_id_type=MESH,
        )

    def a_copy(it, r):
        mm, gg = place(r)
        return pltpu.make_async_remote_copy(
            src_ref=sums.at[it, rank],
            dst_ref=sums.at[it, rank],
            send_sem=a_send.at[r],
            recv_sem=a_recv.at[r],
            device_id=device(mm, gg),
            device_id_type=MESH,
        )

    def o_copy(r):
        mm = lax.rem(m + r, M)
        return pltpu.make_async_remote_copy(
            src_ref=occ.at[m],
            dst_ref=occ.at[m],
            send_sem=o_send.at[r],
            recv_sem=o_recv.at[r],
            device_id=device(mm, g),
            device_id_type=MESH,
        )

    def g_copy(which, r):
        mm = lax.rem(m + r, M)
        return pltpu.make_async_remote_copy(
            src_ref=gath.at[which, m],
            dst_ref=gath.at[which, m],
            send_sem=g_send.at[which, r],
            recv_sem=g_recv.at[which, r],
            device_id=device(mm, g),
            device_id_type=MESH,
        )

    def start_all(make, count):
        def body(r, _):
            make(r).start()
            return 0

        lax.fori_loop(1, count, body, 0)

    def wait_sent(make, count):
        def body(r, _):
            make(r).wait_send()
            return 0

        lax.fori_loop(1, count, body, 0)

    def wait_arrived(make, count):
        def body(r, _):
            make(r).wait_recv()
            return 0

        lax.fori_loop(1, count, body, 0)

    def forward_zy(t, per_block):
        def body(j, _):
            place_of = j if per_block else 0
            for two in range(PL // 2):
                rows = []
                for q in (2 * two, 2 * two + 1):
                    f = fac[place_of, q]
                    real = (psi[t, j, 0, q].astype(F32) * f).astype(BF)
                    imag = (psi[t, j, 1, q].astype(F32) * f).astype(BF)
                    rows.append(jnp.concatenate([real, imag], axis=1))
                along = dot(jnp.concatenate(rows, axis=0), fz[...]).astype(BF)
                top = jnp.concatenate([along[:NG, :NG], along[NG:, :NG]], axis=1)
                low = jnp.concatenate([along[:NG, NG:], along[NG:, NG:]], axis=1)
                out = dot(fy[...], jnp.concatenate([top, low], axis=0)).astype(BF)
                for side in range(2):
                    for gg in range(G):
                        send_f[t, gg, j, 2 * two + side] = out[
                            gg * C : (gg + 1) * C, side * NG : (side + 1) * NG
                        ]
            return 0

        lax.fori_loop(0, M, body, 0)

    def spectral(t):
        def spread(blk, _):
            gg, mm = blk // M, lax.rem(blk, M)
            for p in range(PL):
                start = pl.multiple_of((blk * PL + p) * xs, 8)
                xscr[pl.ds(start, C), :] = recv_f[t, gg, mm, p].astype(F32)
            return 0

        lax.fori_loop(0, peers, spread, 0)
        unroll = min(4, C)

        def columns(part, _):
            for two in range(unroll // 2):
                stacked = []
                for side in range(2):
                    kl = part * unroll + two * 2 + side
                    x = xscr[pl.ds(kl, NG, stride=xs), :]
                    stacked.append(jnp.concatenate([x.astype(BF), rot(x).astype(BF)], axis=0))
                c = dot(fy[...], jnp.concatenate(stacked, axis=1))
                stacked = []
                for side in range(2):
                    kl = part * unroll + two * 2 + side
                    damp = pair_damp[...] * single_damp[pl.ds(g * C + kl, 1), :]
                    one = c[:, side * NG : (side + 1) * NG] * damp
                    stacked.append(jnp.concatenate([one.astype(BF), rot(one).astype(BF)], axis=0))
                d = dot(iy[...], jnp.concatenate(stacked, axis=1))
                for side in range(2):
                    kl = part * unroll + two * 2 + side
                    start = pl.multiple_of(kl * ds, 8)
                    dscr[pl.ds(start, NG), :] = d[:, side * NG : (side + 1) * NG]
            return 0

        lax.fori_loop(0, C // unroll, columns, 0)

        def collect(blk, _):
            gg, mm = blk // M, lax.rem(blk, M)
            for p in range(PL):
                v = dscr[pl.ds(blk * PL + p, C, stride=ds), :]
                send_b[p // PB, gg, mm, p % PB, t] = v.astype(BF)
            return 0

        lax.fori_loop(0, peers, collect, 0)

    def inverse_yz(it, k):
        keep = it < ITERS - 1

        def body(pp, _):
            p = k * PB + pp
            total = jnp.zeros((NG, NG), F32)
            for j in range(M):
                stacked = []
                for t in range(NB):
                    d = jnp.concatenate(
                        [recv_b[k, j, gg, pp, t].astype(F32) for gg in range(G)], axis=0
                    )
                    stacked.append(jnp.concatenate([d.astype(BF), rot(d).astype(BF)], axis=0))
                e = dot(iy[...], jnp.concatenate(stacked, axis=1)).astype(BF)
                e = jnp.concatenate([e[:, t * NG : (t + 1) * NG] for t in range(NB)], axis=0)
                wave = dot(e, iz[...]).astype(BF)
                for t in range(NB):
                    real = wave[t * NG : (t + 1) * NG, :NG]
                    imag = wave[t * NG : (t + 1) * NG, NG:]
                    if keep:
                        psi[t, j, 0, p] = real
                        psi[t, j, 1, p] = imag
                    real = real.astype(F32)
                    imag = imag.astype(F32)
                    total = total + occ[j, t] * (real * real + imag * imag)
            parts[it, h, p] = (total * (density_scale / (NB * M * H))).astype(BF)
            return 0

        lax.fori_loop(0, PB, body, 0)

    for t in range(NB):
        occ[m, t] = jnp.full((1, NG), occ_in[t], F32)

    for copy in first:
        copy.wait()

    def first_factor(j, _):
        for q in range(PL):
            plane = j * PL + q
            fac[j, q] = jnp.exp(-time_step * (ext[plane] + coupling * rho0[plane] - energy_shift))
        return 0

    lax.fori_loop(0, M, first_factor, 0)

    cells = 1.0 / (NG * NG * NG)
    for it in range(ITERS):
        slot = (DEPTH - 1 + it) % DEPTH
        forward_make = f1_copy if it == 0 else f_copy
        forward_count = G if it == 0 else peers
        for t in range(NB):
            if it > 0:
                wait_sent(functools.partial(f1_copy if it == 1 else f_copy, t), G if it == 1 else peers)
            forward_zy(t, it == 0)
            if it == 0 and t == 0:
                pl.semaphore_wait(barrier, peers - 1 + H - 1)
                start_all(o_copy, M)
            start_all(functools.partial(forward_make, t), forward_count)
            if it == 0:
                recv_f[t, g] = send_f[t, g]
            else:
                recv_f[t, g, m] = send_f[t, g, m]
        if it == 0:
            for copy in later:
                copy.wait()

            def prepare(p, accs):
                entries = [q_hist[j, p] for j in range(DEPTH - 1)]
                out = list(accs)
                for j in range(DEPTH - 1):
                    t_hist[j, p] = t_hist[j, p] + mixing_weight * entries[j]
                    for kk in range(j + 1):
                        out[spot(j, kk)] = out[spot(j, kk)] + fold(entries[j] * entries[kk])
                return tuple(out)

            zeros = tuple(jnp.zeros((8, NG), F32) for _ in range(spot(DEPTH - 1, 0)))
            kept_sums = lax.fori_loop(0, PL, prepare, zeros)
            line = jnp.zeros((1, NG), F32)
            for n, acc in enumerate(kept_sums):
                value = jnp.sum(jnp.sum(acc, axis=0, keepdims=True), axis=1, keepdims=True)
                line = line + jnp.where(lane == 2 * DEPTH + n, value, 0.0)
            gsc[0] = line
        for t in range(NB):
            wait_arrived(functools.partial(forward_make, t), forward_count)
            if it > 0 and t == 0:
                for k in range(K):
                    wait_sent(functools.partial(b_copy, k), peers)
            spectral(t)
        for k in range(K):
            start_all(functools.partial(b_copy, k), peers)
            recv_b[k, m, g] = send_b[k, g, m]
        if it == 0:
            wait_arrived(o_copy, M)
        for k in range(K):
            wait_arrived(functools.partial(b_copy, k), peers)
            inverse_yz(it, k)
            start_all(functools.partial(e_copy, it, k), H)

        accs = tuple(jnp.zeros((8, NG), F32) for _ in range(2 * DEPTH))
        for k in range(K):
            wait_arrived(functools.partial(e_copy, it, k), H)

            def gather_sums(p, accs, it=it, slot=slot):
                rho = parts[it, 0, p].astype(F32)
                for hh in range(1, H):
                    rho = rho + parts[it, hh, p].astype(F32)
                before = prev[p] if it == 0 else now[it - 1, p]
                here = now[it, p]
                residual = rho - here
                newest = residual - res[it, p]
                res[it + 1, p] = residual
                q_hist[slot, p] = newest
                t_hist[slot, p] = (here - before) + mixing_weight * newest
                out = list(accs)
                for j in range(DEPTH):
                    entry = newest if j == slot else q_hist[j, p]
                    out[j] = out[j] + fold(entry * newest)
                    out[DEPTH + j] = out[DEPTH + j] + fold(entry * residual)
                if it == ITERS - 1:
                    gath[1, m, p] = residual.astype(BF)
                return tuple(out)

            accs = lax.fori_loop(k * PB, (k + 1) * PB, gather_sums, accs)
        if it == ITERS - 1:
            start_all(functools.partial(g_copy, 1), M)
        line = gsc[0] if it == 0 else jnp.zeros((1, NG), F32)
        for n, acc in enumerate(accs):
            value = jnp.sum(jnp.sum(acc, axis=0, keepdims=True), axis=1, keepdims=True)
            line = line + jnp.where(lane == n, value, 0.0)
        if it > 0:
            wait_sent(functools.partial(a_copy, it - 1), peers)
        sums[it, rank] = line
        start_all(functools.partial(a_copy, it), peers)
        wait_arrived(functools.partial(a_copy, it), peers)
        total = sums[it, 0]
        for r in range(1, peers):
            total = total + sums[it, r]
        total = total * cells

        def pick(n):
            value = jnp.sum(jnp.where(lane == n, total, 0.0), axis=1, keepdims=True)
            return jnp.broadcast_to(value, (1, NG))

        if it == 0:
            for n in range(spot(DEPTH - 1, 0)):
                gsc[1 + n] = pick(2 * DEPTH + n)
        vector = [pick(DEPTH + j) for j in range(DEPTH)]
        for j in range(DEPTH):
            gsc[1 + spot(j, slot)] = pick(j)
        gram = {(j, kk): gsc[1 + spot(j, kk)] for j in range(DEPTH) for kk in range(j + 1)}
        coeffs = solve(gram, vector)

        def mix(p, _, it=it, coeffs=coeffs):
            value = now[it, p] + mixing_weight * res[it + 1, p]
            for j in range(DEPTH):
                value = value - coeffs[j] * t_hist[j, p]
            if it == ITERS - 1:
                gath[0, m, p] = value.astype(BF)
            else:
                now[it + 1, p] = value
                own = ext[m * PL + p]
                fac[0, p] = jnp.exp(-time_step * (own + coupling * value - energy_shift))
            return 0

        lax.fori_loop(0, PL, mix, 0)

    start_all(functools.partial(g_copy, 0), M)
    for which, out in ((1, residual_out), (0, density_out)):
        for r in range(M):
            mm = lax.rem(m + M - r, M)
            if r > 0:
                g_copy(which, r).wait_recv()

            def widen(p, _, which=which, mm=mm):
                staged[which, mm, p] = gath[which, mm, p].astype(F32)
                return 0

            lax.fori_loop(0, PL, widen, 0)
            pltpu.make_async_copy(
                staged.at[which, mm], out.at[pl.ds(mm * PL, PL)], out_sem.at[which, r]
            ).start()
    for which, out in ((1, residual_out), (0, density_out)):
        for r in range(M):
            mm = lax.rem(m + M - r, M)
            pltpu.make_async_copy(
                staged.at[which, mm], out.at[pl.ds(mm * PL, PL)], out_sem.at[which, r]
            ).wait()

    for t in range(NB):
        wait_sent(functools.partial(f_copy, t), peers)
    for k in range(K):
        wait_sent(functools.partial(b_copy, k), peers)
        for it in range(ITERS):
            wait_sent(functools.partial(e_copy, it, k), H)
    wait_sent(functools.partial(a_copy, ITERS - 1), peers)
    wait_sent(o_copy, M)
    for which in range(2):
        wait_sent(functools.partial(g_copy, which), M)


def solution(mesh):
    G = mesh.shape["grid"]
    B = mesh.shape["band"]

    def local(
        bands,
        occupations,
        external,
        density_in,
        prev_density,
        prev_residual,
        hist_density,
        hist_residual,
    ):
        NB = bands.shape[1]
        S, NG = external.shape[0], external.shape[1]
        M = max(1, min(B, S // 8))
        H = B // M
        PL = S // M
        C = NG // 2 // G
        K = min(4, PL)
        PB = PL // K
        dims = (G, M, H, NB, PL, C, K, PB, NG)
        peers = G * M
        hbm = pl.BlockSpec(memory_space=pl.ANY)
        vmem = pl.BlockSpec(memory_space=pltpu.VMEM)
        smem = pl.BlockSpec(memory_space=pltpu.SMEM)
        field = jax.ShapeDtypeStruct((S, NG, NG), F32)
        dma = pltpu.SemaphoreType.DMA
        loads = 2 + NB * M * 2 + 3 + 2 * (DEPTH - 1)
        scratch = [
            pltpu.VMEM((NB, M, 2, PL, NG, NG), BF),
            pltpu.VMEM((NB, G, M, PL, C, NG), BF),
            pltpu.VMEM((NB, G, M, PL, C, NG), BF),
            pltpu.VMEM((K, G, M, PB, NB, C, NG), BF),
            pltpu.VMEM((K, M, G, PB, NB, C, NG), BF),
            pltpu.VMEM((NG * (C + 8), NG), F32),
            pltpu.VMEM((C * (NG + 8), NG), F32),
            pltpu.VMEM((M, PL, NG, NG), F32),
            pltpu.VMEM((S, NG, NG), F32),
            pltpu.VMEM((S, NG, NG), F32),
            pltpu.VMEM((DEPTH, PL, NG, NG), F32),
            pltpu.VMEM((DEPTH, PL, NG, NG), F32),
            pltpu.VMEM((ITERS, PL, NG, NG), F32),
            pltpu.VMEM((ITERS + 1, PL, NG, NG), F32),
            pltpu.VMEM((PL, NG, NG), F32),
            pltpu.VMEM((ITERS, H, PL, NG, NG), BF),
            pltpu.VMEM((ITERS, peers, 1, NG), F32),
            pltpu.VMEM((1 + DEPTH * (DEPTH + 1) // 2, 1, NG), F32),
            pltpu.VMEM((M, NB, 1, NG), F32),
            pltpu.VMEM((2, M, PL, NG, NG), BF),
            pltpu.VMEM((2, M, PL, NG, NG), F32),
            dma((loads,)),
            dma((NB, G)),
            dma((NB, G)),
            dma((NB, peers)),
            dma((NB, peers)),
            dma((K, peers)),
            dma((K, peers)),
            dma((ITERS, K, H)),
            dma((ITERS, K, H)),
            dma((peers,)),
            dma((peers,)),
            dma((M,)),
            dma((M,)),
            dma((2, M)),
            dma((2, M)),
            dma((2, M)),
        ]
        return pl.pallas_call(
            functools.partial(kernel, dims),
            in_specs=[smem] + [hbm] * 7 + [vmem] * 6,
            out_specs=(hbm, hbm),
            out_shape=(field, field),
            scratch_shapes=scratch,
            compiler_params=pltpu.CompilerParams(
                collective_id=0, has_side_effects=True, vmem_limit_bytes=60 * 1024 * 1024
            ),
            name="scf",
        )(
            occupations,
            bands,
            external,
            density_in,
            prev_density,
            prev_residual,
            hist_density,
            hist_residual,
            *make_tables(NG),
        )

    placed = (
        P(None, "band", "grid", None, None),
        P("band"),
        P("grid", None, None),
        P("grid", None, None),
        P("grid", None, None),
        P("grid", None, None),
        P(None, "grid", None, None),
        P(None, "grid", None, None),
    )
    return jax.shard_map(
        local,
        mesh=mesh,
        in_specs=placed,
        out_specs=(P("grid", None, None), P("grid", None, None)),
        check_vma=False,
    )
```

```python
import contextlib
import functools
import math

import jax
import jax.numpy as jnp
import numpy as np
from jax import lax
from jax.experimental import pallas as pl
from jax.experimental.pallas import tpu as pltpu
from jax.sharding import PartitionSpec as P

DEPTH = 6
ITERS = 3

time_step = 0.25
energy_shift = 2.5
coupling = 1.0
mixing_weight = 0.5
ridge_share = 0.1
ridge_floor = 0.01
density_scale = 8.0

MESH = pl.DeviceIdType.MESH


def mark(name):
    return contextlib.nullcontext()

BF = jnp.bfloat16
F32 = jnp.float32


def make_tables(ng):
    freq = np.arange(-(ng // 4), ng // 4)
    phase = (np.arange(ng)[:, None] * freq[None, :]) % ng
    angles = phase.astype(np.float64) * (2.0 * math.pi / ng)
    cos = (np.cos(angles) / math.sqrt(ng)).astype(np.float32)
    sin = (np.sin(angles) / math.sqrt(ng)).astype(np.float32)
    forward_z = np.concatenate(
        [np.concatenate([cos, -sin, -sin, -cos], 1), np.concatenate([sin, cos, cos, -sin], 1)], 0
    )
    forward = np.concatenate([cos.T, sin.T], 1)
    forward_x = np.concatenate([cos.T, sin.T], 0)
    inverse = np.concatenate([cos, -sin], 1)
    inverse_z = np.concatenate(
        [np.concatenate([cos.T, sin.T], 1), np.concatenate([-sin.T, cos.T], 1)], 0
    )
    quarter = ng / 4.0
    damp = np.exp(-time_step * (freq.astype(np.float64) ** 2) / (quarter * quarter))
    damp = damp * ((freq >= -(ng // 4)) & (freq < ng // 4))
    pair = damp[:, None] * np.concatenate([damp, damp])[None, :]
    single = np.broadcast_to(damp[:, None], (damp.shape[0], 2 * damp.shape[0]))
    as_bf = lambda table: jnp.asarray(table, F32).astype(BF)
    return (
        as_bf(forward_z),
        as_bf(forward),
        as_bf(forward_x),
        as_bf(inverse),
        as_bf(inverse_z),
        jnp.asarray(pair, F32),
        jnp.asarray(np.ascontiguousarray(single), F32),
    )


def dot(a, b):
    return jnp.dot(a, b, preferred_element_type=F32)


def fold(cells):
    return jnp.sum(cells.reshape(-1, 8, cells.shape[-1]), axis=0)


def spot(j, k):
    return (j * (j + 1) // 2 + k) if j >= k else (k * (k + 1) // 2 + j)


def solve(gram, vector):
    trace = gram[0, 0]
    for j in range(1, DEPTH):
        trace = trace + gram[j, j]
    ridge = trace * (ridge_share / DEPTH) + ridge_floor
    matrix = {(j, k): gram[j, k] + ridge if j == k else gram[j, k] for (j, k) in gram}
    vector = list(vector)
    inverse = []
    for k in range(DEPTH):
        inverse.append(1.0 / matrix[k, k])
        scaled = {j: matrix[j, k] * inverse[k] for j in range(k + 1, DEPTH)}
        for j in range(k + 1, DEPTH):
            vector[j] = vector[j] - scaled[j] * vector[k]
            for m in range(k + 1, j + 1):
                matrix[j, m] = matrix[j, m] - scaled[j] * matrix[m, k]
    for k in reversed(range(DEPTH)):
        value = vector[k]
        for j in range(k + 1, DEPTH):
            value = value - matrix[j, k] * vector[j]
        vector[k] = value * inverse[k]
    return vector


def kernel(
    dims,
    occ_in,
    bands,
    external,
    density_in,
    prev_density,
    prev_residual,
    hist_density,
    hist_residual,
    fz,
    fy,
    fx,
    iy,
    iz,
    pair_damp,
    single_damp,
    density_out,
    residual_out,
    psi,
    send_f,
    recv_f,
    send_b,
    recv_b,
    along_z,
    xscr,
    xrhs,
    crhs,
    dscr,
    drhs,
    erows,
    fac,
    ext,
    rho0,
    q_hist,
    t_hist,
    now,
    res,
    prev,
    parts,
    sums,
    gsc,
    occ,
    gath,
    load_sem,
    f_send,
    f_recv,
    b_send,
    b_recv,
    e_send,
    e_recv,
    a_send,
    a_recv,
    o_send,
    o_recv,
    g_send,
    g_recv,
    out_sem,
):
    G, M, H, NB, PL, C, K, PB, NG = dims
    kept = C * G
    peers = G * M
    xs = C + 8
    ds = NG + 8
    g = lax.axis_index("grid")
    b = lax.axis_index("band")
    m = lax.rem(b, M)
    h = b // M
    rank = m * G + g

    def place(r):
        other = lax.rem(rank + r, peers)
        return other // G, lax.rem(other, G)

    def source(r):
        other = lax.rem(rank + peers - r, peers)
        return other // G, lax.rem(other, G)

    def device(mm, gg):
        return (h * M + mm, gg)

    loads = []

    def load(src, dst):
        copy = pltpu.make_async_copy(src, dst, load_sem.at[len(loads)])
        copy.start()
        loads.append(copy)
        return copy

    first = []
    for t in range(NB):
        group = []
        for j in range(M):
            block = pl.ds(j * PL, PL)
            if t == 0:
                group.append(load(external.at[block], ext.at[block]))
                group.append(load(density_in.at[block], rho0.at[block]))
            for c in range(2):
                group.append(load(bands.at[c, t, block], psi.at[t, j, :, :, pl.ds(c * NG, NG)]))
        first.append(group)
    mine = pl.ds(m * PL, PL)
    later = [
        load(density_in.at[mine], now.at[0]),
        load(prev_density.at[mine], prev),
        load(prev_residual.at[mine], res.at[0]),
    ]
    for j in range(DEPTH - 1):
        later.append(load(hist_residual.at[j, mine], q_hist.at[j]))
        later.append(load(hist_density.at[j, mine], t_hist.at[j]))

    barrier = pltpu.get_barrier_semaphore()

    def greet(r, _):
        mm, gg = place(r)
        pl.semaphore_signal(barrier, inc=1, device_id=device(mm, gg), device_id_type=MESH)
        return 0

    lax.fori_loop(1, peers, greet, 0)

    def greet_half(r, _):
        hh = lax.rem(h + r, H)
        pl.semaphore_signal(barrier, inc=1, device_id=(hh * M + m, g), device_id_type=MESH)
        return 0

    lax.fori_loop(1, H, greet_half, 0)

    lane = lax.broadcasted_iota(jnp.int32, (1, NG), 1)
    sign = jnp.where(lane < NG // 2, 1.0, -1.0).astype(F32)

    def rot(x):
        return pltpu.roll(x, NG // 2, 1) * sign

    def f_copy(t, gg, j, slot, mm):
        return pltpu.make_async_remote_copy(
            src_ref=send_f.at[t, gg * M + j],
            dst_ref=recv_f.at[t, slot],
            send_sem=f_send.at[t, gg * M + j],
            recv_sem=f_recv.at[t, slot],
            device_id=device(mm, gg),
            device_id_type=MESH,
        )

    own = g * M + m

    def f_arrived(it, t):
        lowest = M if it == 0 else 1
        base = g * M if it == 0 else own

        def body(r, _):
            slot = lax.rem(base + r, peers)
            f_copy(t, slot // M, lax.rem(slot, M), slot, m).wait_recv()
            return 0

        lax.fori_loop(lowest, peers, body, 0)

    def f_sent(it, t):
        lowest = M if it == 0 else 1
        base = g * M if it == 0 else own

        def body(r, _):
            slot = lax.rem(base + r, peers)
            f_copy(t, slot // M, lax.rem(slot, M), slot, m).wait_send()
            return 0

        lax.fori_loop(lowest, peers, body, 0)

    def b_copy(k, r):
        mm, gg = place(r)
        return pltpu.make_async_remote_copy(
            src_ref=send_b.at[k, gg, mm],
            dst_ref=recv_b.at[k, m, g],
            send_sem=b_send.at[k, r],
            recv_sem=b_recv.at[k, r],
            device_id=device(mm, gg),
            device_id_type=MESH,
        )

    def e_copy(it, k, r):
        hh = lax.rem(h + r, H)
        rows = pl.ds(k * PB, PB)
        return pltpu.make_async_remote_copy(
            src_ref=parts.at[it, h, rows],
            dst_ref=parts.at[it, h, rows],
            send_sem=e_send.at[it, k, r],
            recv_sem=e_recv.at[it, k, r],
            device_id=(hh * M + m, g),
            device_id_type=MESH,
        )

    def a_copy(it, r):
        mm, gg = place(r)
        return pltpu.make_async_remote_copy(
            src_ref=sums.at[it, rank],
            dst_ref=sums.at[it, rank],
            send_sem=a_send.at[r],
            recv_sem=a_recv.at[r],
            device_id=device(mm, gg),
            device_id_type=MESH,
        )

    def o_copy(r):
        mm = lax.rem(m + r, M)
        return pltpu.make_async_remote_copy(
            src_ref=occ.at[m],
            dst_ref=occ.at[m],
            send_sem=o_send.at[r],
            recv_sem=o_recv.at[r],
            device_id=device(mm, g),
            device_id_type=MESH,
        )

    def g_copy(which, k, r):
        mm = lax.rem(m + r, M)
        rows = pl.ds(k * PB, PB)
        return pltpu.make_async_remote_copy(
            src_ref=gath.at[which, m, rows],
            dst_ref=gath.at[which, m, rows],
            send_sem=g_send.at[which, k, r],
            recv_sem=g_recv.at[which, k, r],
            device_id=device(mm, g),
            device_id_type=MESH,
        )

    def start_all(make, count):
        def body(r, _):
            make(r).start()
            return 0

        lax.fori_loop(1, count, body, 0)

    def wait_sent(make, count):
        def body(r, _):
            make(r).wait_send()
            return 0

        lax.fori_loop(1, count, body, 0)

    def wait_arrived(make, count):
        def body(r, _):
            make(r).wait_recv()
            return 0

        lax.fori_loop(1, count, body, 0)

    def forward_zy(it, t):
        def make(j):
            at = j if it == 0 else 0
            for q in range(PL):
                f = fac[at, q]
                real = (psi[t, j, q, :, :NG].astype(F32) * f).astype(BF)
                imag = (psi[t, j, q, :, NG:].astype(F32) * f).astype(BF)
                along_z[q] = dot(jnp.concatenate([real, imag], axis=1), fz[...]).astype(BF)
            for two in range(PL // 2):
                even, odd = along_z[2 * two], along_z[2 * two + 1]
                top = jnp.concatenate([even[:, :NG], odd[:, :NG]], axis=1)
                low = jnp.concatenate([even[:, NG:], odd[:, NG:]], axis=1)
                out = dot(fy[...], jnp.concatenate([top, low], axis=0)).astype(BF)
                for side in range(2):
                    for gg in range(G):
                        send_f[t, gg * M + j, 2 * two + side] = out[
                            gg * C : (gg + 1) * C, side * NG : (side + 1) * NG
                        ]

        def send(j, lowest):
            def body(r, _):
                gg = lax.rem(g + r, G)
                if it == 0:
                    f_copy(t, gg, j, g * M + j, m).start()
                else:
                    f_copy(t, gg, j, own, j).start()
                return 0

            lax.fori_loop(lowest, G, body, 0)

        def step(n, _):
            j = lax.rem(m + 1 + n, M)
            make(j)
            send(j, 1 if it == 0 else 0)
            if it == 0:
                recv_f[t, g * M + j] = send_f[t, g * M + j]
            return 0

        if it == 0:
            lax.fori_loop(0, M, step, 0)
        else:
            lax.fori_loop(0, M - 1, step, 0)
            make(m)
            send(m, 1)
            recv_f[t, own] = send_f[t, own]

    def spectral(t):
        def spread(blk, _):
            for p in range(PL):
                start = pl.multiple_of((blk * PL + p) * xs, 8)
                xscr[pl.ds(start, C), :] = recv_f[t, blk, p].astype(F32)
            return 0

        lax.fori_loop(0, peers, spread, 0)
        for kl in range(C):
            xrhs[:, kl * NG : (kl + 1) * NG] = xscr[pl.ds(kl, NG, stride=xs), :].astype(BF)
        for two in range(C // 2):
            c = dot(fx[...], xrhs[:, two * 2 * NG : (two + 1) * 2 * NG])
            for side in range(2):
                kl = 2 * two + side
                lanes = slice(side * NG, (side + 1) * NG)
                damp = pair_damp[...] * single_damp[pl.ds(g * C + kl, 1), :]
                one = (c[:kept, lanes] + rot(c[kept:, lanes])) * damp
                crhs[:kept, kl * NG : (kl + 1) * NG] = one.astype(BF)
                crhs[kept:, kl * NG : (kl + 1) * NG] = rot(one).astype(BF)
        for two in range(C // 2):
            d = dot(iy[...], crhs[:, two * 2 * NG : (two + 1) * 2 * NG])
            for side in range(2):
                kl = 2 * two + side
                dscr[kl * ds : kl * ds + NG, :] = d[:, side * NG : (side + 1) * NG]

    def collect(t, k):
        def body(blk, _):
            for pp in range(PB):
                v = dscr[pl.ds(blk * PL + k * PB + pp, C, stride=ds), :]
                send_b[k, blk // M, lax.rem(blk, M), pp, t] = v.astype(BF)
            return 0

        lax.fori_loop(0, peers, body, 0)

    def inverse_yz(it, k):
        def body(pp, _):
            p = k * PB + pp
            count = NB * M
            for n in range(count):
                d = jnp.concatenate(
                    [recv_b[k, n // NB, gg, pp, n % NB].astype(F32) for gg in range(G)], axis=0
                )
                drhs[:kept, n * NG : (n + 1) * NG] = d.astype(BF)
                drhs[kept:, n * NG : (n + 1) * NG] = rot(d).astype(BF)
            for two in range(count // 2):
                e = dot(iy[...], drhs[:, two * 2 * NG : (two + 1) * 2 * NG]).astype(BF)
                for side in range(2):
                    n = 2 * two + side
                    erows[n * NG : (n + 1) * NG, :] = e[:, side * NG : (side + 1) * NG]
            for n in range(count):
                psi[n % NB, n // NB, p] = dot(erows[n * NG : (n + 1) * NG, :], iz[...]).astype(BF)
            total = jnp.zeros((NG, NG), F32)
            for n in range(count):
                real = psi[n % NB, n // NB, p, :, :NG].astype(F32)
                imag = psi[n % NB, n // NB, p, :, NG:].astype(F32)
                total = total + occ[n // NB, n % NB] * (real * real + imag * imag)
            parts[it, h, p] = (total * (density_scale / (NB * M * H))).astype(BF)
            return 0

        lax.fori_loop(0, PB, body, 0)

    for t in range(NB):
        occ[m, t] = jnp.full((1, NG), occ_in[t], F32)

    with mark("loads"):
        for copy in first[0]:
            copy.wait()

    def first_factor(j, _):
        for q in range(PL):
            plane = j * PL + q
            fac[j, q] = jnp.exp(-time_step * (ext[plane] + coupling * rho0[plane] - energy_shift))
        return 0

    with mark("factor"):
        lax.fori_loop(0, M, first_factor, 0)
    with mark("barrier"):
        pl.semaphore_wait(barrier, peers - 1 + H - 1)
    start_all(o_copy, M)

    cells = 1.0 / (NG * NG * NG)
    for it in range(ITERS):
        slot = (DEPTH - 1 + it) % DEPTH
        for t in range(NB):
            if it == 0 and t > 0:
                for copy in first[t]:
                    copy.wait()
            with mark(f"F{t}"):
                forward_zy(it, t)
        if it == 0:
            with mark("later"):
                for copy in later:
                    copy.wait()

            def prepare(p, accs):
                entries = [q_hist[j, p] for j in range(DEPTH - 1)]
                out = list(accs)
                for j in range(DEPTH - 1):
                    t_hist[j, p] = t_hist[j, p] + mixing_weight * entries[j]
                    for kk in range(j + 1):
                        out[spot(j, kk)] = out[spot(j, kk)] + fold(entries[j] * entries[kk])
                return tuple(out)

            zeros = tuple(jnp.zeros((8, NG), F32) for _ in range(spot(DEPTH - 1, 0)))
            with mark("prepare"):
                kept_sums = lax.fori_loop(0, PL, prepare, zeros)
            line = jnp.zeros((1, NG), F32)
            for n, acc in enumerate(kept_sums):
                value = jnp.sum(jnp.sum(acc, axis=0, keepdims=True), axis=1, keepdims=True)
                line = line + jnp.where(lane == 2 * DEPTH + n, value, 0.0)
            gsc[0] = line
        for t in range(NB):
            with mark(f"waitF{t}"):
                f_arrived(it, t)
            with mark(f"X{t}"):
                spectral(t)
            for k in range(K):
                with mark(f"collect{t}{k}"):
                    collect(t, k)
                    if t == NB - 1:
                        start_all(functools.partial(b_copy, k), peers)
                        recv_b[k, m, g] = send_b[k, g, m]
        for t in range(NB):
            f_sent(it, t)
        if it == 0:
            wait_arrived(o_copy, M)
        for k in range(K):
            with mark(f"waitB{k}"):
                wait_arrived(functools.partial(b_copy, k), peers)
            with mark(f"C{k}"):
                inverse_yz(it, k)
            start_all(functools.partial(e_copy, it, k), H)

        accs = tuple(jnp.zeros((8, NG), F32) for _ in range(2 * DEPTH))
        for k in range(K):
            with mark(f"waitE{k}"):
                wait_arrived(functools.partial(e_copy, it, k), H)

            def gather_sums(p, accs, it=it, slot=slot):
                rho = parts[it, 0, p].astype(F32)
                for hh in range(1, H):
                    rho = rho + parts[it, hh, p].astype(F32)
                before = prev[p] if it == 0 else now[it - 1, p]
                here = now[it, p]
                residual = rho - here
                newest = residual - res[it, p]
                res[it + 1, p] = residual
                q_hist[slot, p] = newest
                t_hist[slot, p] = (here - before) + mixing_weight * newest
                out = list(accs)
                for j in range(DEPTH):
                    entry = newest if j == slot else q_hist[j, p]
                    out[j] = out[j] + fold(entry * newest)
                    out[DEPTH + j] = out[DEPTH + j] + fold(entry * residual)
                if it == ITERS - 1:
                    gath[1, m, p] = residual.astype(BF)
                return tuple(out)

            with mark(f"gram{k}"):
                accs = lax.fori_loop(k * PB, (k + 1) * PB, gather_sums, accs)
            if it == ITERS - 1 and k < K - 1:
                start_all(functools.partial(g_copy, 1, k), M)
        line = gsc[0] if it == 0 else jnp.zeros((1, NG), F32)
        for n, acc in enumerate(accs):
            value = jnp.sum(jnp.sum(acc, axis=0, keepdims=True), axis=1, keepdims=True)
            line = line + jnp.where(lane == n, value, 0.0)
        sums[it, rank] = line
        start_all(functools.partial(a_copy, it), peers)
        if it == ITERS - 1:
            start_all(functools.partial(g_copy, 1, K - 1), M)
        for k in range(K):
            wait_sent(functools.partial(b_copy, k), peers)
            wait_sent(functools.partial(e_copy, it, k), H)
        with mark("waitA"):
            wait_arrived(functools.partial(a_copy, it), peers)
        total = sums[it, 0]
        for r in range(1, peers):
            total = total + sums[it, r]
        total = total * cells

        def pick(n):
            value = jnp.sum(jnp.where(lane == n, total, 0.0), axis=1, keepdims=True)
            return jnp.broadcast_to(value, (1, NG))

        if it == 0:
            for n in range(spot(DEPTH - 1, 0)):
                gsc[1 + n] = pick(2 * DEPTH + n)
        vector = [pick(DEPTH + j) for j in range(DEPTH)]
        for j in range(DEPTH):
            gsc[1 + spot(j, slot)] = pick(j)
        gram = {(j, kk): gsc[1 + spot(j, kk)] for j in range(DEPTH) for kk in range(j + 1)}
        with mark("solve"):
            coeffs = solve(gram, vector)

        def mix(p, _, it=it, coeffs=coeffs):
            value = now[it, p] + mixing_weight * res[it + 1, p]
            for j in range(DEPTH):
                value = value - coeffs[j] * t_hist[j, p]
            if it == ITERS - 1:
                gath[0, m, p] = value.astype(BF)
            else:
                now[it + 1, p] = value
                own = ext[m * PL + p]
                fac[0, p] = jnp.exp(-time_step * (own + coupling * value - energy_shift))
            return 0

        wait_sent(functools.partial(a_copy, it), peers)
        with mark("mix"):
            for k in range(K):
                lax.fori_loop(k * PB, (k + 1) * PB, mix, 0)
                if it == ITERS - 1:
                    start_all(functools.partial(g_copy, 0, k), M)

    def out_copy(which, r):
        mm = lax.rem(m + M - r, M)
        out = density_out if which == 0 else residual_out
        return pltpu.make_async_copy(
            gath.at[which, mm], out.at[pl.ds(mm * PL, PL)], out_sem.at[which, r]
        )

    for which in (1, 0):
        for r in range(M):
            if r > 0:
                with mark(f"waitG{which}{r}"):
                    for k in range(K):
                        g_copy(which, k, r).wait_recv()
            out_copy(which, r).start()
    for which in (1, 0):
        for r in range(M):
            out_copy(which, r).wait()
    wait_sent(o_copy, M)
    for which in range(2):
        for k in range(K):
            wait_sent(functools.partial(g_copy, which, k), M)


def solution(mesh):
    G = mesh.shape["grid"]
    B = mesh.shape["band"]

    def local(
        bands,
        occupations,
        external,
        density_in,
        prev_density,
        prev_residual,
        hist_density,
        hist_residual,
    ):
        NB = bands.shape[1]
        S, NG = external.shape[0], external.shape[1]
        M = max(1, min(B, S // 8))
        H = B // M
        PL = S // M
        C = NG // 2 // G
        K = min(4, PL)
        PB = PL // K
        dims = (G, M, H, NB, PL, C, K, PB, NG)
        peers = G * M
        hbm = pl.BlockSpec(memory_space=pl.ANY)
        vmem = pl.BlockSpec(memory_space=pltpu.VMEM)
        smem = pl.BlockSpec(memory_space=pltpu.SMEM)
        field = jax.ShapeDtypeStruct((S, NG, NG), BF)
        dma = pltpu.SemaphoreType.DMA
        loads = 2 * M + NB * M * 2 + 3 + 2 * (DEPTH - 1)
        bands_held = NB * M
        scratch = [
            pltpu.VMEM((NB, M, PL, NG, 2 * NG), BF),
            pltpu.VMEM((NB, peers, PL, C, NG), BF),
            pltpu.VMEM((NB, peers, PL, C, NG), BF),
            pltpu.VMEM((K, G, M, PB, NB, C, NG), BF),
            pltpu.VMEM((K, M, G, PB, NB, C, NG), BF),
            pltpu.VMEM((PL, NG, 2 * NG), BF),
            pltpu.VMEM((NG * (C + 8), NG), F32),
            pltpu.VMEM((NG, C * NG), BF),
            pltpu.VMEM((NG, C * NG), BF),
            pltpu.VMEM((C * (NG + 8), NG), F32),
            pltpu.VMEM((NG, bands_held * NG), BF),
            pltpu.VMEM((bands_held * NG, NG), BF),
            pltpu.VMEM((M, PL, NG, NG), F32),
            pltpu.VMEM((S, NG, NG), F32),
            pltpu.VMEM((S, NG, NG), F32),
            pltpu.VMEM((DEPTH, PL, NG, NG), F32),
            pltpu.VMEM((DEPTH, PL, NG, NG), F32),
            pltpu.VMEM((ITERS, PL, NG, NG), F32),
            pltpu.VMEM((ITERS + 1, PL, NG, NG), F32),
            pltpu.VMEM((PL, NG, NG), F32),
            pltpu.VMEM((ITERS, H, PL, NG, NG), BF),
            pltpu.VMEM((ITERS, peers, 1, NG), F32),
            pltpu.VMEM((1 + DEPTH * (DEPTH + 1) // 2, 1, NG), F32),
            pltpu.VMEM((M, NB, 1, NG), F32),
            pltpu.VMEM((2, M, PL, NG, NG), BF),
            dma((loads,)),
            dma((NB, peers)),
            dma((NB, peers)),
            dma((K, peers)),
            dma((K, peers)),
            dma((ITERS, K, H)),
            dma((ITERS, K, H)),
            dma((peers,)),
            dma((peers,)),
            dma((M,)),
            dma((M,)),
            dma((2, K, M)),
            dma((2, K, M)),
            dma((2, M)),
        ]
        density, residual = pl.pallas_call(
            functools.partial(kernel, dims),
            in_specs=[smem] + [hbm] * 7 + [vmem] * 7,
            out_specs=(hbm, hbm),
            out_shape=(field, field),
            scratch_shapes=scratch,
            compiler_params=pltpu.CompilerParams(
                collective_id=0, has_side_effects=True, vmem_limit_bytes=60 * 1024 * 1024
            ),
            name="scf",
        )(
            occupations,
            bands,
            external,
            density_in,
            prev_density,
            prev_residual,
            hist_density,
            hist_residual,
            *make_tables(NG),
        )
        return density.astype(F32), residual.astype(F32)

    placed = (
        P(None, "band", "grid", None, None),
        P("band"),
        P("grid", None, None),
        P("grid", None, None),
        P("grid", None, None),
        P("grid", None, None),
        P(None, "grid", None, None),
        P(None, "grid", None, None),
    )
    return jax.shard_map(
        local,
        mesh=mesh,
        in_specs=placed,
        out_specs=(P("grid", None, None), P("grid", None, None)),
        check_vma=False,
    )
```

```python
import contextlib
import functools
import math

import jax
import jax.numpy as jnp
import numpy as np
from jax import lax
from jax.experimental import pallas as pl
from jax.experimental.pallas import tpu as pltpu
from jax.sharding import PartitionSpec as P

DEPTH = 6
ITERS = 3

time_step = 0.25
energy_shift = 2.5
coupling = 1.0
mixing_weight = 0.5
ridge_share = 0.1
ridge_floor = 0.01
density_scale = 8.0

MESH = pl.DeviceIdType.MESH


def mark(name):
    return contextlib.nullcontext()

BF = jnp.bfloat16
F32 = jnp.float32


def make_tables(ng):
    freq = np.arange(-(ng // 4), ng // 4)
    phase = (np.arange(ng)[:, None] * freq[None, :]) % ng
    angles = phase.astype(np.float64) * (2.0 * math.pi / ng)
    cos = (np.cos(angles) / math.sqrt(ng)).astype(np.float32)
    sin = (np.sin(angles) / math.sqrt(ng)).astype(np.float32)
    forward_z = np.concatenate(
        [np.concatenate([cos, -sin, -sin, -cos], 1), np.concatenate([sin, cos, cos, -sin], 1)], 0
    )
    forward = np.concatenate([cos.T, sin.T], 1)
    forward_x = np.concatenate([cos.T, sin.T], 0)
    inverse = np.concatenate([cos, -sin], 1)
    inverse_z = np.concatenate(
        [np.concatenate([cos.T, sin.T], 1), np.concatenate([-sin.T, cos.T], 1)], 0
    )
    quarter = ng / 4.0
    damp = np.exp(-time_step * (freq.astype(np.float64) ** 2) / (quarter * quarter))
    damp = damp * ((freq >= -(ng // 4)) & (freq < ng // 4))
    pair = damp[:, None] * np.concatenate([damp, damp])[None, :]
    single = np.broadcast_to(damp[:, None], (damp.shape[0], 2 * damp.shape[0]))
    as_bf = lambda table: jnp.asarray(table, F32).astype(BF)
    return (
        as_bf(forward_z),
        as_bf(forward),
        as_bf(forward_x),
        as_bf(inverse),
        as_bf(inverse_z),
        jnp.asarray(pair, F32),
        jnp.asarray(np.ascontiguousarray(single), F32),
    )


def dot(a, b):
    return jnp.dot(a, b, preferred_element_type=F32)


def fold(cells):
    return jnp.sum(cells.reshape(-1, 8, cells.shape[-1]), axis=0)


def spot(j, k):
    return (j * (j + 1) // 2 + k) if j >= k else (k * (k + 1) // 2 + j)


def solve(gram, vector):
    trace = gram[0, 0]
    for j in range(1, DEPTH):
        trace = trace + gram[j, j]
    ridge = trace * (ridge_share / DEPTH) + ridge_floor
    matrix = {(j, k): gram[j, k] + ridge if j == k else gram[j, k] for (j, k) in gram}
    vector = list(vector)
    inverse = []
    for k in range(DEPTH):
        inverse.append(1.0 / matrix[k, k])
        scaled = {j: matrix[j, k] * inverse[k] for j in range(k + 1, DEPTH)}
        for j in range(k + 1, DEPTH):
            vector[j] = vector[j] - scaled[j] * vector[k]
            for m in range(k + 1, j + 1):
                matrix[j, m] = matrix[j, m] - scaled[j] * matrix[m, k]
    for k in reversed(range(DEPTH)):
        value = vector[k]
        for j in range(k + 1, DEPTH):
            value = value - matrix[j, k] * vector[j]
        vector[k] = value * inverse[k]
    return vector


def kernel(
    dims,
    occ_in,
    bands,
    external,
    density_in,
    prev_density,
    prev_residual,
    hist_density,
    hist_residual,
    fz_in,
    fy_in,
    fx_in,
    iy_in,
    iz_in,
    pair_in,
    single_in,
    density_out,
    residual_out,
    fz,
    fy,
    fx,
    iy,
    iz,
    pair_damp,
    single_damp,
    psi,
    send_f,
    recv_f,
    send_b,
    recv_b,
    along_z,
    xscr,
    xrhs,
    crhs,
    dscr,
    drhs,
    erows,
    fac,
    ext,
    rho0,
    q_hist,
    t_hist,
    now,
    res,
    prev,
    parts,
    sums,
    gsc,
    occ,
    gath,
    table_sem,
    field_sem,
    band_sem,
    load_sem,
    f_send,
    f_recv,
    b_send,
    b_recv,
    e_send,
    e_recv,
    a_send,
    a_recv,
    o_send,
    o_recv,
    g_send,
    g_recv,
    r_send,
    r_recv,
    out_sem,
):
    G, M, H, NB, PL, C, K, PB, GK, NG = dims
    GP = PL // GK
    relay = M == 4 and GP % 2 == 0
    kept = C * G
    peers = G * M
    xs = C + 8
    ds = NG + 8
    g = lax.axis_index("grid")
    b = lax.axis_index("band")
    m = lax.rem(b, M)
    h = b // M
    rank = m * G + g

    def place(r):
        other = lax.rem(rank + r, peers)
        return other // G, lax.rem(other, G)

    def source(r):
        other = lax.rem(rank + peers - r, peers)
        return other // G, lax.rem(other, G)

    def device(mm, gg):
        return (h * M + mm, gg)

    loads = []

    def load(src, dst):
        copy = pltpu.make_async_copy(src, dst, load_sem.at[len(loads)])
        copy.start()
        loads.append(copy)
        return copy

    tables = [
        pltpu.make_async_copy(src, dst, table_sem.at[n])
        for n, (src, dst) in enumerate(
            (
                (fz_in, fz),
                (fy_in, fy),
                (fx_in, fx),
                (iy_in, iy),
                (iz_in, iz),
                (pair_in, pair_damp),
                (single_in, single_damp),
            )
        )
    ]

    def field_load(n, i):
        block = pl.ds(lax.rem(m + 1 + n, M) * PL, PL)
        src, dst = ((external, ext), (density_in, rho0))[i]
        return pltpu.make_async_copy(src.at[block], dst.at[block], field_sem.at[i, n])

    def band_load(t, n, c):
        j = lax.rem(m + 1 + n, M)
        return pltpu.make_async_copy(
            bands.at[c, t, pl.ds(j * PL, PL)],
            psi.at[t, j, :, :, pl.ds(c * NG, NG)],
            band_sem.at[t, c, n],
        )

    for n in range(M):
        field_load(n, 0).start()
        field_load(n, 1).start()
        band_load(0, n, 0).start()
        band_load(0, n, 1).start()
        if n == 0:
            for copy in tables:
                copy.start()
    for t in range(1, NB):
        for n in range(M):
            for c in range(2):
                band_load(t, n, c).start()
    mine = pl.ds(m * PL, PL)
    later = [
        load(density_in.at[mine], now.at[0]),
        load(prev_density.at[mine], prev),
        load(prev_residual.at[mine], res.at[0]),
    ]
    for j in range(DEPTH - 1):
        later.append(load(hist_residual.at[j, mine], q_hist.at[j]))
        later.append(load(hist_density.at[j, mine], t_hist.at[j]))

    barrier = pltpu.get_barrier_semaphore()

    def greet(r, _):
        mm, gg = place(r)
        pl.semaphore_signal(barrier, inc=1, device_id=device(mm, gg), device_id_type=MESH)
        return 0

    lax.fori_loop(1, peers, greet, 0)

    def greet_half(r, _):
        hh = lax.rem(h + r, H)
        pl.semaphore_signal(barrier, inc=1, device_id=(hh * M + m, g), device_id_type=MESH)
        return 0

    lax.fori_loop(1, H, greet_half, 0)

    lane = lax.broadcasted_iota(jnp.int32, (1, NG), 1)
    sign = jnp.where(lane < NG // 2, 1.0, -1.0).astype(F32)

    def rot(x):
        return pltpu.roll(x, NG // 2, 1) * sign

    lanes8 = lax.broadcasted_iota(jnp.int32, (8, NG), 1)

    def in_lanes(accs, offset):
        rows = jnp.zeros((8, NG), F32)
        for n, acc in enumerate(accs):
            rows = rows + jnp.where(lanes8 == offset + n, jnp.sum(acc, axis=1, keepdims=True), 0.0)
        return jnp.sum(rows, axis=0, keepdims=True)

    def f_copy(t, gg, j, slot, mm):
        return pltpu.make_async_remote_copy(
            src_ref=send_f.at[t, gg * M + j],
            dst_ref=recv_f.at[t, slot],
            send_sem=f_send.at[t, gg * M + j],
            recv_sem=f_recv.at[t, slot],
            device_id=device(mm, gg),
            device_id_type=MESH,
        )

    own = g * M + m

    def f_arrived(it, t):
        lowest = M if it == 0 else 1
        base = g * M if it == 0 else own

        def body(r, _):
            slot = lax.rem(base + r, peers)
            f_copy(t, slot // M, lax.rem(slot, M), slot, m).wait_recv()
            return 0

        lax.fori_loop(lowest, peers, body, 0)

    def f_sent(it, t):
        lowest = M if it == 0 else 1
        base = g * M if it == 0 else own

        def body(r, _):
            slot = lax.rem(base + r, peers)
            f_copy(t, slot // M, lax.rem(slot, M), slot, m).wait_send()
            return 0

        lax.fori_loop(lowest, peers, body, 0)

    def b_copy(k, r):
        mm, gg = place(r)
        return pltpu.make_async_remote_copy(
            src_ref=send_b.at[k, gg, mm],
            dst_ref=recv_b.at[k, m, g],
            send_sem=b_send.at[k, r],
            recv_sem=b_recv.at[k, r],
            device_id=device(mm, gg),
            device_id_type=MESH,
        )

    def e_copy(it, k, r):
        hh = lax.rem(h + r, H)
        rows = pl.ds(k * PB, PB)
        return pltpu.make_async_remote_copy(
            src_ref=parts.at[it, h, rows],
            dst_ref=parts.at[it, h, rows],
            send_sem=e_send.at[it, k, r],
            recv_sem=e_recv.at[it, k, r],
            device_id=(hh * M + m, g),
            device_id_type=MESH,
        )

    def a_copy(it, r):
        mm, gg = place(r)
        return pltpu.make_async_remote_copy(
            src_ref=sums.at[it, rank],
            dst_ref=sums.at[it, rank],
            send_sem=a_send.at[r],
            recv_sem=a_recv.at[r],
            device_id=device(mm, gg),
            device_id_type=MESH,
        )

    def o_copy(r):
        mm = lax.rem(m + r, M)
        return pltpu.make_async_remote_copy(
            src_ref=occ.at[m],
            dst_ref=occ.at[m],
            send_sem=o_send.at[r],
            recv_sem=o_recv.at[r],
            device_id=device(mm, g),
            device_id_type=MESH,
        )

    def near(r):
        if not relay:
            return lax.rem(m + r, M)
        return m + 1 - 2 * lax.rem(m, 2) if r == 1 else lax.rem(m + 2, M)

    direct = (1, 2) if relay else tuple(range(1, M))

    def g_copy(which, k, r):
        rows = pl.ds(k * GP, GP)
        return pltpu.make_async_remote_copy(
            src_ref=gath.at[which, m, rows],
            dst_ref=gath.at[which, m, rows],
            send_sem=g_send.at[which, k, r],
            recv_sem=g_recv.at[which, k, r],
            device_id=device(near(r), g),
            device_id_type=MESH,
        )

    def r_copy(which, k, r):
        rows = pl.ds(k * GP + (r - 1) * (GP // 2), GP // 2)
        block = near(r)
        return pltpu.make_async_remote_copy(
            src_ref=gath.at[which, block, rows],
            dst_ref=gath.at[which, block, rows],
            send_sem=r_send.at[which, k, r],
            recv_sem=r_recv.at[which, k, r],
            device_id=device(near(3 - r), g),
            device_id_type=MESH,
        )

    def g_start(which, k):
        for r in direct:
            g_copy(which, k, r).start()

    def g_pass_on(which, k):
        for r in direct:
            if relay:
                g_copy(which, k, r).wait_recv()
                r_copy(which, k, r).start()

    def start_all(make, count):
        def body(r, _):
            make(r).start()
            return 0

        lax.fori_loop(1, count, body, 0)

    def wait_sent(make, count):
        def body(r, _):
            make(r).wait_send()
            return 0

        lax.fori_loop(1, count, body, 0)

    def wait_arrived(make, count):
        def body(r, _):
            make(r).wait_recv()
            return 0

        lax.fori_loop(1, count, body, 0)

    def forward_zy(it, t):
        def make(j):
            at = j if it == 0 else 0
            for q in range(PL):
                f = fac[at, q]
                real = (psi[t, j, q, :, :NG].astype(F32) * f).astype(BF)
                imag = (psi[t, j, q, :, NG:].astype(F32) * f).astype(BF)
                along_z[q] = dot(jnp.concatenate([real, imag], axis=1), fz[...]).astype(BF)
            for two in range(PL // 2):
                even, odd = along_z[2 * two], along_z[2 * two + 1]
                top = jnp.concatenate([even[:, :NG], odd[:, :NG]], axis=1)
                low = jnp.concatenate([even[:, NG:], odd[:, NG:]], axis=1)
                out = dot(fy[...], jnp.concatenate([top, low], axis=0)).astype(BF)
                for side in range(2):
                    for gg in range(G):
                        send_f[t, gg * M + j, 2 * two + side] = out[
                            gg * C : (gg + 1) * C, side * NG : (side + 1) * NG
                        ]

        def send(j, lowest):
            def body(r, _):
                gg = lax.rem(g + r, G)
                if it == 0:
                    f_copy(t, gg, j, g * M + j, m).start()
                else:
                    f_copy(t, gg, j, own, j).start()
                return 0

            lax.fori_loop(lowest, G, body, 0)

        def step(n, _):
            j = lax.rem(m + 1 + n, M)
            if it == 0:
                band_load(t, n, 0).wait()
                band_load(t, n, 1).wait()
            if it == 0 and t == 0:
                field_load(n, 0).wait()
                field_load(n, 1).wait()
                for q in range(PL):
                    plane = j * PL + q
                    fac[j, q] = jnp.exp(
                        -time_step * (ext[plane] + coupling * rho0[plane] - energy_shift)
                    )
            make(j)
            send(j, 1 if it == 0 else 0)
            if it == 0:
                recv_f[t, g * M + j] = send_f[t, g * M + j]
            return 0

        if it == 0:
            lax.fori_loop(0, M, step, 0)
        else:
            lax.fori_loop(0, M - 1, step, 0)
            make(m)
            send(m, 1)
            recv_f[t, own] = send_f[t, own]

    def spectral(t):
        def spread(blk, _):
            for p in range(PL):
                start = pl.multiple_of((blk * PL + p) * xs, 8)
                xscr[pl.ds(start, C), :] = recv_f[t, blk, p].astype(F32)
            return 0

        lax.fori_loop(0, peers, spread, 0)
        for kl in range(C):
            xrhs[:, kl * NG : (kl + 1) * NG] = xscr[pl.ds(kl, NG, stride=xs), :].astype(BF)
        for two in range(C // 2):
            c = dot(fx[...], xrhs[:, two * 2 * NG : (two + 1) * 2 * NG])
            for side in range(2):
                kl = 2 * two + side
                lanes = slice(side * NG, (side + 1) * NG)
                damp = pair_damp[...] * single_damp[pl.ds(g * C + kl, 1), :]
                one = (c[:kept, lanes] + rot(c[kept:, lanes])) * damp
                crhs[:kept, kl * NG : (kl + 1) * NG] = one.astype(BF)
                crhs[kept:, kl * NG : (kl + 1) * NG] = rot(one).astype(BF)
        for two in range(C // 2):
            d = dot(iy[...], crhs[:, two * 2 * NG : (two + 1) * 2 * NG])
            for side in range(2):
                kl = 2 * two + side
                dscr[kl * ds : kl * ds + NG, :] = d[:, side * NG : (side + 1) * NG]

    def collect(t, lowest, count):
        def body(blk, _):
            for p in range(lowest, lowest + count):
                v = dscr[pl.ds(blk * PL + p, C, stride=ds), :]
                send_b[p // PB, blk // M, lax.rem(blk, M), p % PB, t] = v.astype(BF)
            return 0

        lax.fori_loop(0, peers, body, 0)

    def inverse_yz(it, k):
        def body(pp, _):
            p = k * PB + pp
            count = NB * M
            for n in range(count):
                d = jnp.concatenate(
                    [recv_b[k, n // NB, gg, pp, n % NB].astype(F32) for gg in range(G)], axis=0
                )
                drhs[:kept, n * NG : (n + 1) * NG] = d.astype(BF)
                drhs[kept:, n * NG : (n + 1) * NG] = rot(d).astype(BF)
            for two in range(count // 2):
                e = dot(iy[...], drhs[:, two * 2 * NG : (two + 1) * 2 * NG]).astype(BF)
                for side in range(2):
                    n = 2 * two + side
                    erows[n * NG : (n + 1) * NG, :] = e[:, side * NG : (side + 1) * NG]
            for n in range(count):
                psi[n % NB, n // NB, p] = dot(erows[n * NG : (n + 1) * NG, :], iz[...]).astype(BF)
            total = jnp.zeros((NG, NG), F32)
            for n in range(count):
                real = psi[n % NB, n // NB, p, :, :NG].astype(F32)
                imag = psi[n % NB, n // NB, p, :, NG:].astype(F32)
                total = total + occ[n // NB, n % NB] * (real * real + imag * imag)
            parts[it, h, p] = (total * (density_scale / (NB * M * H))).astype(BF)
            return 0

        lax.fori_loop(0, PB, body, 0)

    for t in range(NB):
        occ[m, t] = jnp.full((1, NG), occ_in[t], F32)

    for copy in tables:
        copy.wait()
    with mark("barrier"):
        pl.semaphore_wait(barrier, peers - 1 + H - 1)
    start_all(o_copy, M)

    cells = 1.0 / (NG * NG * NG)
    for it in range(ITERS):
        slot = (DEPTH - 1 + it) % DEPTH
        for t in range(NB):
            with mark(f"F{t}"):
                forward_zy(it, t)
        if it == 0:
            with mark("later"):
                for copy in later:
                    copy.wait()

            def prepare(p, accs):
                entries = [q_hist[j, p] for j in range(DEPTH - 1)]
                out = list(accs)
                for j in range(DEPTH - 1):
                    t_hist[j, p] = t_hist[j, p] + mixing_weight * entries[j]
                    for kk in range(j + 1):
                        out[spot(j, kk)] = out[spot(j, kk)] + fold(entries[j] * entries[kk])
                return tuple(out)

            zeros = tuple(jnp.zeros((8, NG), F32) for _ in range(spot(DEPTH - 1, 0)))
            with mark("prepare"):
                kept_sums = lax.fori_loop(0, PL, prepare, zeros)
            gsc[0] = in_lanes(kept_sums, 2 * DEPTH)
        for t in range(NB):
            with mark(f"waitF{t}"):
                f_arrived(it, t)
            with mark(f"X{t}"):
                spectral(t)
            with mark(f"collect{t}"):
                if t < NB - 1:
                    collect(t, 0, PL)
                else:
                    for k in range(K):
                        collect(t, k * PB, PB)
                        start_all(functools.partial(b_copy, k), peers)
                        recv_b[k, m, g] = send_b[k, g, m]
        if it == 0:
            wait_arrived(o_copy, M)
        for k in range(K):
            with mark(f"waitB{k}"):
                wait_arrived(functools.partial(b_copy, k), peers)
            with mark(f"C{k}"):
                inverse_yz(it, k)
            start_all(functools.partial(e_copy, it, k), H)

        accs = tuple(jnp.zeros((8, NG), F32) for _ in range(2 * DEPTH))
        for k in range(K):
            with mark(f"waitE{k}"):
                wait_arrived(functools.partial(e_copy, it, k), H)

            def gather_sums(p, accs, it=it, slot=slot):
                rho = parts[it, 0, p].astype(F32)
                for hh in range(1, H):
                    rho = rho + parts[it, hh, p].astype(F32)
                before = prev[p] if it == 0 else now[it - 1, p]
                here = now[it, p]
                residual = rho - here
                newest = residual - res[it, p]
                res[it + 1, p] = residual
                q_hist[slot, p] = newest
                t_hist[slot, p] = (here - before) + mixing_weight * newest
                out = list(accs)
                for j in range(DEPTH):
                    entry = newest if j == slot else q_hist[j, p]
                    out[j] = out[j] + fold(entry * newest)
                    out[DEPTH + j] = out[DEPTH + j] + fold(entry * residual)
                if it == ITERS - 1:
                    gath[1, m, p] = residual.astype(BF)
                return tuple(out)

            with mark(f"gram{k}"):
                accs = lax.fori_loop(k * PB, (k + 1) * PB, gather_sums, accs)
            ready = (k + 1) * PB
            if it == ITERS - 1 and ready % GP == 0 and ready < PL:
                g_start(1, ready // GP - 1)
        line = in_lanes(accs, 0)
        sums[it, rank] = gsc[0] + line if it == 0 else line
        start_all(functools.partial(a_copy, it), peers)
        if it == ITERS - 1:
            g_start(1, GK - 1)
            for k in range(GK - 2):
                g_pass_on(1, k)
        for t in range(NB):
            f_sent(it, t)
        for k in range(K):
            wait_sent(functools.partial(b_copy, k), peers)
            wait_sent(functools.partial(e_copy, it, k), H)
        with mark("waitA"):
            wait_arrived(functools.partial(a_copy, it), peers)
        total = sums[it, 0]
        for r in range(1, peers):
            total = total + sums[it, r]
        total = total * cells

        def pick(n):
            value = jnp.sum(jnp.where(lane == n, total, 0.0), axis=1, keepdims=True)
            return jnp.broadcast_to(value, (1, NG))

        if it == 0:
            for n in range(spot(DEPTH - 1, 0)):
                gsc[1 + n] = pick(2 * DEPTH + n)
        vector = [pick(DEPTH + j) for j in range(DEPTH)]
        for j in range(DEPTH):
            gsc[1 + spot(j, slot)] = pick(j)
        gram = {(j, kk): gsc[1 + spot(j, kk)] for j in range(DEPTH) for kk in range(j + 1)}
        with mark("solve"):
            coeffs = solve(gram, vector)

        def mix(p, _, it=it, coeffs=coeffs):
            value = now[it, p] + mixing_weight * res[it + 1, p]
            for j in range(DEPTH):
                value = value - coeffs[j] * t_hist[j, p]
            if it == ITERS - 1:
                gath[0, m, p] = value.astype(BF)
            else:
                now[it + 1, p] = value
                own = ext[m * PL + p]
                fac[0, p] = jnp.exp(-time_step * (own + coupling * value - energy_shift))
            return 0

        wait_sent(functools.partial(a_copy, it), peers)
        with mark("mix"):
            for k in range(GK):
                lax.fori_loop(k * GP, (k + 1) * GP, mix, 0)
                if it == ITERS - 1:
                    g_start(0, k)

    def out_copy(which, block):
        out = density_out if which == 0 else residual_out
        return pltpu.make_async_copy(
            gath.at[which, block], out.at[pl.ds(block * PL, PL)], out_sem.at[which, block]
        )

    with mark("pass"):
        for k in range(max(GK - 2, 0), GK):
            g_pass_on(1, k)
        for k in range(GK):
            g_pass_on(0, k)
    for which in (1, 0):
        out_copy(which, m).start()
        for r in direct:
            if not relay:
                for k in range(GK):
                    g_copy(which, k, r).wait_recv()
            out_copy(which, near(r)).start()
        if relay:
            with mark(f"waitR{which}"):
                for k in range(GK):
                    for r in direct:
                        r_copy(which, k, r).wait_recv()
            out_copy(which, 3 - m).start()
    for which in (1, 0):
        for block in range(M):
            out_copy(which, block).wait()
    wait_sent(o_copy, M)
    for which in range(2):
        for k in range(GK):
            for r in direct:
                g_copy(which, k, r).wait_send()
                if relay:
                    r_copy(which, k, r).wait_send()


def widen_kernel(blocks, density, residual, density_out, residual_out, narrow, wide, in_sem, out_sem):
    rows = density.shape[0] // blocks
    sources = (density, residual)
    targets = (density_out, residual_out)
    steps = [(w, pl.ds(n * rows, rows), n) for n in range(blocks) for w in range(2)]
    for w, part, n in steps:
        pltpu.make_async_copy(sources[w].at[part], narrow.at[w, part], in_sem.at[w, n]).start()
    for w, part, n in steps:
        pltpu.make_async_copy(sources[w].at[part], narrow.at[w, part], in_sem.at[w, n]).wait()
        wide[w, part] = narrow[w, part].astype(F32)
        pltpu.make_async_copy(wide.at[w, part], targets[w].at[part], out_sem.at[w, n]).start()
    for w, part, n in steps:
        pltpu.make_async_copy(wide.at[w, part], targets[w].at[part], out_sem.at[w, n]).wait()


def widen(density, residual):
    blocks = min(4, density.shape[0])
    hbm = pl.BlockSpec(memory_space=pl.ANY)
    field = jax.ShapeDtypeStruct(density.shape, F32)
    return pl.pallas_call(
        functools.partial(widen_kernel, blocks),
        in_specs=[hbm] * 2,
        out_specs=(hbm, hbm),
        out_shape=(field, field),
        scratch_shapes=[
            pltpu.VMEM((2,) + density.shape, BF),
            pltpu.VMEM((2,) + density.shape, F32),
            pltpu.SemaphoreType.DMA((2, blocks)),
            pltpu.SemaphoreType.DMA((2, blocks)),
        ],
        name="widen",
    )(density, residual)


def solution(mesh):
    G = mesh.shape["grid"]
    B = mesh.shape["band"]

    def local(
        bands,
        occupations,
        external,
        density_in,
        prev_density,
        prev_residual,
        hist_density,
        hist_residual,
    ):
        NB = bands.shape[1]
        S, NG = external.shape[0], external.shape[1]
        M = max(1, min(B, S // 8))
        H = B // M
        PL = S // M
        C = NG // 2 // G
        K = PL
        PB = PL // K
        GK = min(4, PL)
        dims = (G, M, H, NB, PL, C, K, PB, GK, NG)
        peers = G * M
        hbm = pl.BlockSpec(memory_space=pl.ANY)
        smem = pl.BlockSpec(memory_space=pltpu.SMEM)
        field = jax.ShapeDtypeStruct((S, NG, NG), BF)
        dma = pltpu.SemaphoreType.DMA
        loads = 3 + 2 * (DEPTH - 1)
        tables = make_tables(NG)
        bands_held = NB * M
        scratch = [pltpu.VMEM(table.shape, table.dtype) for table in tables] + [
            pltpu.VMEM((NB, M, PL, NG, 2 * NG), BF),
            pltpu.VMEM((NB, peers, PL, C, NG), BF),
            pltpu.VMEM((NB, peers, PL, C, NG), BF),
            pltpu.VMEM((K, G, M, PB, NB, C, NG), BF),
            pltpu.VMEM((K, M, G, PB, NB, C, NG), BF),
            pltpu.VMEM((PL, NG, 2 * NG), BF),
            pltpu.VMEM((NG * (C + 8), NG), F32),
            pltpu.VMEM((NG, C * NG), BF),
            pltpu.VMEM((NG, C * NG), BF),
            pltpu.VMEM((C * (NG + 8), NG), F32),
            pltpu.VMEM((NG, bands_held * NG), BF),
            pltpu.VMEM((bands_held * NG, NG), BF),
            pltpu.VMEM((M, PL, NG, NG), F32),
            pltpu.VMEM((S, NG, NG), F32),
            pltpu.VMEM((S, NG, NG), F32),
            pltpu.VMEM((DEPTH, PL, NG, NG), F32),
            pltpu.VMEM((DEPTH, PL, NG, NG), F32),
            pltpu.VMEM((ITERS, PL, NG, NG), F32),
            pltpu.VMEM((ITERS + 1, PL, NG, NG), F32),
            pltpu.VMEM((PL, NG, NG), F32),
            pltpu.VMEM((ITERS, H, PL, NG, NG), BF),
            pltpu.VMEM((ITERS, peers, 1, NG), F32),
            pltpu.VMEM((1 + DEPTH * (DEPTH + 1) // 2, 1, NG), F32),
            pltpu.VMEM((M, NB, 1, NG), F32),
            pltpu.VMEM((2, M, PL, NG, NG), BF),
            dma((len(tables),)),
            dma((2, M)),
            dma((NB, 2, M)),
            dma((loads,)),
            dma((NB, peers)),
            dma((NB, peers)),
            dma((K, peers)),
            dma((K, peers)),
            dma((ITERS, K, H)),
            dma((ITERS, K, H)),
            dma((peers,)),
            dma((peers,)),
            dma((M,)),
            dma((M,)),
            dma((2, GK, M)),
            dma((2, GK, M)),
            dma((2, GK, M)),
            dma((2, GK, M)),
            dma((2, M)),
        ]
        density, residual = pl.pallas_call(
            functools.partial(kernel, dims),
            in_specs=[smem] + [hbm] * (7 + len(tables)),
            out_specs=(hbm, hbm),
            out_shape=(field, field),
            scratch_shapes=scratch,
            compiler_params=pltpu.CompilerParams(
                collective_id=0, has_side_effects=True, vmem_limit_bytes=60 * 1024 * 1024
            ),
            name="scf",
        )(
            occupations,
            bands,
            external,
            density_in,
            prev_density,
            prev_residual,
            hist_density,
            hist_residual,
            *tables,
        )
        return widen(density, residual)

    placed = (
        P(None, "band", "grid", None, None),
        P("band"),
        P("grid", None, None),
        P("grid", None, None),
        P("grid", None, None),
        P("grid", None, None),
        P(None, "grid", None, None),
        P(None, "grid", None, None),
    )
    return jax.shard_map(
        local,
        mesh=mesh,
        in_specs=placed,
        out_specs=(P("grid", None, None), P("grid", None, None)),
        check_vma=False,
    )
```

```python
import contextlib
import functools
import math

import jax
import jax.numpy as jnp
import numpy as np
from jax import lax
from jax.experimental import pallas as pl
from jax.experimental.pallas import tpu as pltpu
from jax.sharding import PartitionSpec as P

DEPTH = 6
ITERS = 3

time_step = 0.25
energy_shift = 2.5
coupling = 1.0
mixing_weight = 0.5
ridge_share = 0.1
ridge_floor = 0.01
density_scale = 8.0

MESH = pl.DeviceIdType.MESH


def mark(name):
    return contextlib.nullcontext()

BF = jnp.bfloat16
F32 = jnp.float32


def make_tables(ng):
    freq = np.arange(-(ng // 4), ng // 4)
    phase = (np.arange(ng)[:, None] * freq[None, :]) % ng
    angles = phase.astype(np.float64) * (2.0 * math.pi / ng)
    cos = (np.cos(angles) / math.sqrt(ng)).astype(np.float32)
    sin = (np.sin(angles) / math.sqrt(ng)).astype(np.float32)
    forward_z = np.concatenate(
        [np.concatenate([cos, -sin, -sin, -cos], 1), np.concatenate([sin, cos, cos, -sin], 1)], 0
    )
    forward = np.concatenate([cos.T, sin.T], 1)
    forward_x = np.concatenate([cos.T, sin.T], 0)
    inverse = np.concatenate([cos, -sin], 1)
    inverse_z = np.concatenate(
        [np.concatenate([cos.T, sin.T], 1), np.concatenate([-sin.T, cos.T], 1)], 0
    )
    quarter = ng / 4.0
    damp = np.exp(-time_step * (freq.astype(np.float64) ** 2) / (quarter * quarter))
    damp = damp * ((freq >= -(ng // 4)) & (freq < ng // 4))
    pair = damp[:, None] * np.concatenate([damp, damp])[None, :]
    single = np.broadcast_to(damp[:, None], (damp.shape[0], 2 * damp.shape[0]))
    as_bf = lambda table: jnp.asarray(table, F32).astype(BF)
    return (
        as_bf(forward_z),
        as_bf(forward),
        as_bf(forward_x),
        as_bf(inverse),
        as_bf(inverse_z),
        jnp.asarray(pair, F32),
        jnp.asarray(np.ascontiguousarray(single), F32),
    )


def dot(a, b):
    return jnp.dot(a, b, preferred_element_type=F32)


def fold(cells):
    return jnp.sum(cells.reshape(-1, 8, cells.shape[-1]), axis=0)


def spot(j, k):
    return (j * (j + 1) // 2 + k) if j >= k else (k * (k + 1) // 2 + j)


def solve(gram, vector):
    trace = gram[0, 0]
    for j in range(1, DEPTH):
        trace = trace + gram[j, j]
    ridge = trace * (ridge_share / DEPTH) + ridge_floor
    matrix = {(j, k): gram[j, k] + ridge if j == k else gram[j, k] for (j, k) in gram}
    vector = list(vector)
    inverse = []
    for k in range(DEPTH):
        inverse.append(1.0 / matrix[k, k])
        scaled = {j: matrix[j, k] * inverse[k] for j in range(k + 1, DEPTH)}
        for j in range(k + 1, DEPTH):
            vector[j] = vector[j] - scaled[j] * vector[k]
            for m in range(k + 1, j + 1):
                matrix[j, m] = matrix[j, m] - scaled[j] * matrix[m, k]
    for k in reversed(range(DEPTH)):
        value = vector[k]
        for j in range(k + 1, DEPTH):
            value = value - matrix[j, k] * vector[j]
        vector[k] = value * inverse[k]
    return vector


def kernel(
    dims,
    occ_in,
    bands,
    external,
    density_in,
    prev_density,
    prev_residual,
    hist_density,
    hist_residual,
    fz_in,
    fy_in,
    fx_in,
    iy_in,
    iz_in,
    pair_in,
    single_in,
    density_out,
    residual_out,
    fz,
    fy,
    fx,
    iy,
    iz,
    pair_damp,
    single_damp,
    psi,
    send_f,
    recv_f,
    send_b,
    recv_b,
    along_z,
    xscr,
    xrhs,
    crhs,
    dscr,
    drhs,
    erows,
    fac,
    ext,
    rho0,
    q_hist,
    t_hist,
    now,
    res,
    prev,
    parts,
    sums,
    gsc,
    occ,
    gath,
    table_sem,
    field_sem,
    band_sem,
    load_sem,
    f_send,
    f_recv,
    b_send,
    b_recv,
    e_send,
    e_recv,
    a_send,
    a_recv,
    o_send,
    o_recv,
    g_send,
    g_recv,
    r_send,
    r_recv,
    out_sem,
):
    G, M, H, NB, PL, C, K, PB, GK, NG = dims
    GP = PL // GK
    relay = M == 4 and GP % 2 == 0
    kept = C * G
    peers = G * M
    xs = C + 8
    ds = NG + 8
    g = lax.axis_index("grid")
    b = lax.axis_index("band")
    m = lax.rem(b, M)
    h = b // M
    rank = m * G + g

    def place(r):
        other = lax.rem(rank + r, peers)
        return other // G, lax.rem(other, G)

    def source(r):
        other = lax.rem(rank + peers - r, peers)
        return other // G, lax.rem(other, G)

    def device(mm, gg):
        return (h * M + mm, gg)

    loads = []

    def load(src, dst):
        copy = pltpu.make_async_copy(src, dst, load_sem.at[len(loads)])
        loads.append(copy)
        return copy

    tables = [
        pltpu.make_async_copy(src, dst, table_sem.at[n])
        for n, (src, dst) in enumerate(
            (
                (fz_in, fz),
                (fy_in, fy),
                (fx_in, fx),
                (iy_in, iy),
                (iz_in, iz),
                (pair_in, pair_damp),
                (single_in, single_damp),
            )
        )
    ]

    def field_load(n, i):
        block = pl.ds(lax.rem(m + 1 + n, M) * PL, PL)
        src, dst = ((external, ext), (density_in, rho0))[i]
        return pltpu.make_async_copy(src.at[block], dst.at[block], field_sem.at[i, n])

    def band_load(t, n, c):
        j = lax.rem(m + 1 + n, M)
        return pltpu.make_async_copy(
            bands.at[c, t, pl.ds(j * PL, PL)],
            psi.at[t, j, :, :, pl.ds(c * NG, NG)],
            band_sem.at[t, c, n],
        )

    def start_block(n):
        field_load(n, 0).start()
        field_load(n, 1).start()
        band_load(0, n, 0).start()
        band_load(0, n, 1).start()

    for copy in tables:
        copy.start()
    start_block(0)
    mine = pl.ds(m * PL, PL)
    later = [
        load(density_in.at[mine], now.at[0]),
        load(prev_density.at[mine], prev),
        load(prev_residual.at[mine], res.at[0]),
    ]
    for j in range(DEPTH - 1):
        later.append(load(hist_residual.at[j, mine], q_hist.at[j]))
        later.append(load(hist_density.at[j, mine], t_hist.at[j]))

    barrier = pltpu.get_barrier_semaphore()

    def greet(r, _):
        mm, gg = place(r)
        pl.semaphore_signal(barrier, inc=1, device_id=device(mm, gg), device_id_type=MESH)
        return 0

    lax.fori_loop(1, peers, greet, 0)

    def greet_half(r, _):
        hh = lax.rem(h + r, H)
        pl.semaphore_signal(barrier, inc=1, device_id=(hh * M + m, g), device_id_type=MESH)
        return 0

    lax.fori_loop(1, H, greet_half, 0)

    lane = lax.broadcasted_iota(jnp.int32, (1, NG), 1)
    sign = jnp.where(lane < NG // 2, 1.0, -1.0).astype(F32)

    def rot(x):
        return pltpu.roll(x, NG // 2, 1) * sign

    lanes8 = lax.broadcasted_iota(jnp.int32, (8, NG), 1)

    def in_lanes(accs, offset):
        rows = jnp.zeros((8, NG), F32)
        for n, acc in enumerate(accs):
            rows = rows + jnp.where(lanes8 == offset + n, jnp.sum(acc, axis=1, keepdims=True), 0.0)
        return jnp.sum(rows, axis=0, keepdims=True)

    def f_copy(t, gg, j, slot, mm):
        return pltpu.make_async_remote_copy(
            src_ref=send_f.at[t, gg * M + j],
            dst_ref=recv_f.at[t, slot],
            send_sem=f_send.at[t],
            recv_sem=f_recv.at[t],
            device_id=device(mm, gg),
            device_id_type=MESH,
        )

    own = g * M + m

    def f_all(it, t):
        blocks = pl.ds(0, peers - M if it == 0 else peers - 1)
        mm, gg = place(1)
        return pltpu.make_async_remote_copy(
            src_ref=send_f.at[t, blocks],
            dst_ref=recv_f.at[t, blocks],
            send_sem=f_send.at[t],
            recv_sem=f_recv.at[t],
            device_id=device(mm, gg),
            device_id_type=MESH,
        )

    def b_copy(k, r):
        mm, gg = place(r)
        return pltpu.make_async_remote_copy(
            src_ref=send_b.at[k, gg * M + mm],
            dst_ref=recv_b.at[k, rank],
            send_sem=b_send.at[k],
            recv_sem=b_recv.at[k],
            device_id=device(mm, gg),
            device_id_type=MESH,
        )

    def b_all(k):
        mm, gg = place(1)
        return pltpu.make_async_remote_copy(
            src_ref=send_b.at[k, pl.ds(0, peers - 1)],
            dst_ref=recv_b.at[k, pl.ds(0, peers - 1)],
            send_sem=b_send.at[k],
            recv_sem=b_recv.at[k],
            device_id=device(mm, gg),
            device_id_type=MESH,
        )

    def e_copy(it, k, r):
        hh = lax.rem(h + r, H)
        rows = pl.ds(k * PB, PB)
        return pltpu.make_async_remote_copy(
            src_ref=parts.at[it, h, rows],
            dst_ref=parts.at[it, h, rows],
            send_sem=e_send.at[k],
            recv_sem=e_recv.at[it, k],
            device_id=(hh * M + m, g),
            device_id_type=MESH,
        )

    def e_all(it, k):
        hh = lax.rem(h + 1, H)
        part = parts.at[it, pl.ds(0, H - 1), pl.ds(k * PB, PB)]
        return pltpu.make_async_remote_copy(
            src_ref=part,
            dst_ref=part,
            send_sem=e_send.at[k],
            recv_sem=e_recv.at[it, k],
            device_id=(hh * M + m, g),
            device_id_type=MESH,
        )

    def a_copy(it, r):
        mm, gg = place(r)
        return pltpu.make_async_remote_copy(
            src_ref=sums.at[it, rank],
            dst_ref=sums.at[it, rank],
            send_sem=a_send.at[0],
            recv_sem=a_recv.at[0],
            device_id=device(mm, gg),
            device_id_type=MESH,
        )

    def a_all(it):
        mm, gg = place(1)
        part = sums.at[it, pl.ds(0, peers - 1)]
        return pltpu.make_async_remote_copy(
            src_ref=part,
            dst_ref=part,
            send_sem=a_send.at[0],
            recv_sem=a_recv.at[0],
            device_id=device(mm, gg),
            device_id_type=MESH,
        )

    def o_copy(r):
        mm = lax.rem(m + r, M)
        return pltpu.make_async_remote_copy(
            src_ref=occ.at[m],
            dst_ref=occ.at[m],
            send_sem=o_send.at[0],
            recv_sem=o_recv.at[0],
            device_id=device(mm, g),
            device_id_type=MESH,
        )

    def o_all():
        part = occ.at[pl.ds(0, M - 1)]
        return pltpu.make_async_remote_copy(
            src_ref=part,
            dst_ref=part,
            send_sem=o_send.at[0],
            recv_sem=o_recv.at[0],
            device_id=device(lax.rem(m + 1, M), g),
            device_id_type=MESH,
        )

    def near(r):
        if not relay:
            return lax.rem(m + r, M)
        return m + 1 - 2 * lax.rem(m, 2) if r == 1 else lax.rem(m + 2, M)

    direct = (1, 2) if relay else tuple(range(1, M))

    def g_copy(which, k, r):
        rows = pl.ds(k * GP, GP)
        return pltpu.make_async_remote_copy(
            src_ref=gath.at[which, m, rows],
            dst_ref=gath.at[which, m, rows],
            send_sem=g_send.at[which],
            recv_sem=g_recv.at[which, k, r],
            device_id=device(near(r), g),
            device_id_type=MESH,
        )

    def r_copy(which, k, r):
        rows = pl.ds(k * GP + (r - 1) * (GP // 2), GP // 2)
        block = near(r)
        return pltpu.make_async_remote_copy(
            src_ref=gath.at[which, block, rows],
            dst_ref=gath.at[which, block, rows],
            send_sem=r_send.at[which],
            recv_sem=r_recv.at[which],
            device_id=device(near(3 - r), g),
            device_id_type=MESH,
        )

    def r_all(which):
        return pltpu.make_async_remote_copy(
            src_ref=gath.at[which, 0],
            dst_ref=gath.at[which, 0],
            send_sem=r_send.at[which],
            recv_sem=r_recv.at[which],
            device_id=device(near(1), g),
            device_id_type=MESH,
        )

    def g_all(which):
        part = gath.at[which, pl.ds(0, len(direct))]
        return pltpu.make_async_remote_copy(
            src_ref=part,
            dst_ref=part,
            send_sem=g_send.at[which],
            recv_sem=g_recv.at[which, 0, 0],
            device_id=device(near(1), g),
            device_id_type=MESH,
        )

    def g_start(which, k):
        for r in direct:
            g_copy(which, k, r).start()

    def g_pass_on(which, k):
        for r in direct:
            if relay:
                g_copy(which, k, r).wait_recv()
                r_copy(which, k, r).start()

    def start_all(make, count):
        def body(r, _):
            make(r).start()
            return 0

        lax.fori_loop(1, count, body, 0)

    def forward_zy(it, t):
        def make(j):
            at = j if it == 0 else 0
            for q in range(PL):
                f = fac[at, q]
                real = (psi[t, j, q, :, :NG].astype(F32) * f).astype(BF)
                imag = (psi[t, j, q, :, NG:].astype(F32) * f).astype(BF)
                along_z[q] = dot(jnp.concatenate([real, imag], axis=1), fz[...]).astype(BF)
            for two in range(PL // 2):
                even, odd = along_z[2 * two], along_z[2 * two + 1]
                top = jnp.concatenate([even[:, :NG], odd[:, :NG]], axis=1)
                low = jnp.concatenate([even[:, NG:], odd[:, NG:]], axis=1)
                out = dot(fy[...], jnp.concatenate([top, low], axis=0)).astype(BF)
                for side in range(2):
                    for gg in range(G):
                        send_f[t, gg * M + j, 2 * two + side] = out[
                            gg * C : (gg + 1) * C, side * NG : (side + 1) * NG
                        ]

        def send(j, lowest):
            def body(r, _):
                gg = lax.rem(g + r, G)
                if it == 0:
                    f_copy(t, gg, j, g * M + j, m).start()
                else:
                    f_copy(t, gg, j, own, j).start()
                return 0

            lax.fori_loop(lowest, G, body, 0)

        def step(n, _):
            j = lax.rem(m + 1 + n, M)
            if it == 0 and t == 0:
                for tt in range(1, NB):
                    band_load(tt, n, 0).start()
                    band_load(tt, n, 1).start()

                @pl.when(n + 1 < M)
                def _():
                    start_block(n + 1)

            if it == 0:
                band_load(t, n, 0).wait()
                band_load(t, n, 1).wait()
            if it == 0 and t == 0:
                field_load(n, 0).wait()
                field_load(n, 1).wait()
                for q in range(PL):
                    plane = j * PL + q
                    fac[j, q] = jnp.exp(
                        -time_step * (ext[plane] + coupling * rho0[plane] - energy_shift)
                    )
            make(j)
            send(j, 1 if it == 0 else 0)
            if it == 0:
                recv_f[t, g * M + j] = send_f[t, g * M + j]
            return 0

        if it == 0:
            lax.fori_loop(0, M, step, 0)
            if t == 0:
                for copy in later:
                    copy.start()
        else:
            lax.fori_loop(0, M - 1, step, 0)
            make(m)
            send(m, 1)
            recv_f[t, own] = send_f[t, own]

    def spectral(t):
        def spread(blk, _):
            for p in range(PL):
                start = pl.multiple_of((blk * PL + p) * xs, 8)
                xscr[pl.ds(start, C), :] = recv_f[t, blk, p].astype(F32)
            return 0

        lax.fori_loop(0, peers, spread, 0)
        for kl in range(C):
            xrhs[:, kl * NG : (kl + 1) * NG] = xscr[pl.ds(kl, NG, stride=xs), :].astype(BF)
        for two in range(C // 2):
            c = dot(fx[...], xrhs[:, two * 2 * NG : (two + 1) * 2 * NG])
            for side in range(2):
                kl = 2 * two + side
                lanes = slice(side * NG, (side + 1) * NG)
                damp = pair_damp[...] * single_damp[pl.ds(g * C + kl, 1), :]
                one = (c[:kept, lanes] + rot(c[kept:, lanes])) * damp
                crhs[:kept, kl * NG : (kl + 1) * NG] = one.astype(BF)
                crhs[kept:, kl * NG : (kl + 1) * NG] = rot(one).astype(BF)
        for two in range(C // 2):
            d = dot(iy[...], crhs[:, two * 2 * NG : (two + 1) * 2 * NG])
            for side in range(2):
                kl = 2 * two + side
                dscr[kl * ds : kl * ds + NG, :] = d[:, side * NG : (side + 1) * NG]

    def collect(t, lowest, count):
        def body(blk, _):
            for p in range(lowest, lowest + count):
                v = dscr[pl.ds(blk * PL + p, C, stride=ds), :]
                send_b[p // PB, blk, p % PB, t] = v.astype(BF)
            return 0

        lax.fori_loop(0, peers, body, 0)

    def inverse_yz(it, k):
        def body(pp, _):
            p = k * PB + pp
            count = NB * M
            for n in range(count):
                d = jnp.concatenate(
                    [recv_b[k, n // NB * G + gg, pp, n % NB].astype(F32) for gg in range(G)], axis=0
                )
                drhs[:kept, n * NG : (n + 1) * NG] = d.astype(BF)
                drhs[kept:, n * NG : (n + 1) * NG] = rot(d).astype(BF)
            for two in range(count // 2):
                e = dot(iy[...], drhs[:, two * 2 * NG : (two + 1) * 2 * NG]).astype(BF)
                for side in range(2):
                    n = 2 * two + side
                    erows[n * NG : (n + 1) * NG, :] = e[:, side * NG : (side + 1) * NG]
            for n in range(count):
                psi[n % NB, n // NB, p] = dot(erows[n * NG : (n + 1) * NG, :], iz[...]).astype(BF)
            total = jnp.zeros((NG, NG), F32)
            for n in range(count):
                real = psi[n % NB, n // NB, p, :, :NG].astype(F32)
                imag = psi[n % NB, n // NB, p, :, NG:].astype(F32)
                total = total + occ[n // NB, n % NB] * (real * real + imag * imag)
            parts[it, h, p] = (total * (density_scale / (NB * M * H))).astype(BF)
            return 0

        lax.fori_loop(0, PB, body, 0)

    for t in range(NB):
        occ[m, t] = jnp.full((1, NG), occ_in[t], F32)

    for copy in tables:
        copy.wait()
    with mark("barrier"):
        pl.semaphore_wait(barrier, peers - 1 + H - 1)
    start_all(o_copy, M)

    cells = 1.0 / (NG * NG * NG)
    for it in range(ITERS):
        slot = (DEPTH - 1 + it) % DEPTH
        for t in range(NB):
            with mark(f"F{t}"):
                forward_zy(it, t)
        if it == 0:
            with mark("later"):
                for copy in later:
                    copy.wait()

            def prepare(p, accs):
                entries = [q_hist[j, p] for j in range(DEPTH - 1)]
                out = list(accs)
                for j in range(DEPTH - 1):
                    t_hist[j, p] = t_hist[j, p] + mixing_weight * entries[j]
                    for kk in range(j + 1):
                        out[spot(j, kk)] = out[spot(j, kk)] + fold(entries[j] * entries[kk])
                return tuple(out)

            zeros = tuple(jnp.zeros((8, NG), F32) for _ in range(spot(DEPTH - 1, 0)))
            with mark("prepare"):
                kept_sums = lax.fori_loop(0, PL, prepare, zeros)
            gsc[0] = in_lanes(kept_sums, 2 * DEPTH)
        for t in range(NB):
            with mark(f"waitF{t}"):
                f_all(it, t).wait_recv()
            with mark(f"X{t}"):
                spectral(t)
            with mark(f"collect{t}"):
                if t < NB - 1:
                    collect(t, 0, PL)
                else:
                    for k in range(K):
                        collect(t, k * PB, PB)
                        start_all(functools.partial(b_copy, k), peers)
                        recv_b[k, rank] = send_b[k, own]
        if it == 0 and M > 1:
            o_all().wait_recv()
        for k in range(K):
            with mark(f"waitB{k}"):
                b_all(k).wait_recv()
            with mark(f"C{k}"):
                inverse_yz(it, k)
            start_all(functools.partial(e_copy, it, k), H)

        accs = tuple(jnp.zeros((8, NG), F32) for _ in range(2 * DEPTH))
        for k in range(K):
            with mark(f"waitE{k}"):
                if H > 1:
                    e_all(it, k).wait_recv()

            def gather_sums(p, accs, it=it, slot=slot):
                rho = parts[it, 0, p].astype(F32)
                for hh in range(1, H):
                    rho = rho + parts[it, hh, p].astype(F32)
                before = prev[p] if it == 0 else now[it - 1, p]
                here = now[it, p]
                residual = rho - here
                newest = residual - res[it, p]
                res[it + 1, p] = residual
                q_hist[slot, p] = newest
                t_hist[slot, p] = (here - before) + mixing_weight * newest
                out = list(accs)
                for j in range(DEPTH):
                    entry = newest if j == slot else q_hist[j, p]
                    out[j] = out[j] + fold(entry * newest)
                    out[DEPTH + j] = out[DEPTH + j] + fold(entry * residual)
                if it == ITERS - 1:
                    gath[1, m, p] = residual.astype(BF)
                return tuple(out)

            with mark(f"gram{k}"):
                accs = lax.fori_loop(k * PB, (k + 1) * PB, gather_sums, accs)
            ready = (k + 1) * PB
            if it == ITERS - 1 and ready % GP == 0 and ready < PL:
                g_start(1, ready // GP - 1)
        line = in_lanes(accs, 0)
        sums[it, rank] = gsc[0] + line if it == 0 else line
        start_all(functools.partial(a_copy, it), peers)
        if it == ITERS - 1:
            g_start(1, GK - 1)
            for k in range(GK - 2):
                g_pass_on(1, k)
        for t in range(NB):
            f_all(it, t).wait_send()
        for k in range(K):
            b_all(k).wait_send()
            if H > 1:
                e_all(it, k).wait_send()
        with mark("waitA"):
            a_all(it).wait_recv()
        total = sums[it, 0]
        for r in range(1, peers):
            total = total + sums[it, r]
        total = total * cells

        def pick(n):
            value = jnp.sum(jnp.where(lane == n, total, 0.0), axis=1, keepdims=True)
            return jnp.broadcast_to(value, (1, NG))

        if it == 0:
            for n in range(spot(DEPTH - 1, 0)):
                gsc[1 + n] = pick(2 * DEPTH + n)
        vector = [pick(DEPTH + j) for j in range(DEPTH)]
        for j in range(DEPTH):
            gsc[1 + spot(j, slot)] = pick(j)
        gram = {(j, kk): gsc[1 + spot(j, kk)] for j in range(DEPTH) for kk in range(j + 1)}
        with mark("solve"):
            coeffs = solve(gram, vector)

        def mix(p, _, it=it, coeffs=coeffs):
            value = now[it, p] + mixing_weight * res[it + 1, p]
            for j in range(DEPTH):
                value = value - coeffs[j] * t_hist[j, p]
            if it == ITERS - 1:
                gath[0, m, p] = value.astype(BF)
            else:
                now[it + 1, p] = value
                own = ext[m * PL + p]
                fac[0, p] = jnp.exp(-time_step * (own + coupling * value - energy_shift))
            return 0

        a_all(it).wait_send()
        with mark("mix"):
            for k in range(GK):
                lax.fori_loop(k * GP, (k + 1) * GP, mix, 0)
                if it == ITERS - 1:
                    g_start(0, k)

    def out_copy(which, block):
        out = density_out if which == 0 else residual_out
        return pltpu.make_async_copy(
            gath.at[which, block], out.at[pl.ds(block * PL, PL)], out_sem.at[which, block]
        )

    with mark("pass"):
        for k in range(max(GK - 2, 0), GK):
            g_pass_on(1, k)
        for k in range(GK):
            g_pass_on(0, k)
    for which in (1, 0):
        out_copy(which, m).start()
        for r in direct:
            if not relay:
                for k in range(GK):
                    g_copy(which, k, r).wait_recv()
            out_copy(which, near(r)).start()
        if relay:
            with mark(f"waitR{which}"):
                r_all(which).wait_recv()
            out_copy(which, 3 - m).start()
    with mark("outs"):
        for which in (1, 0):
            for block in range(M):
                out_copy(which, block).wait()
    with mark("drain"):
        if M > 1:
            o_all().wait_send()
        for which in range(2):
            if direct:
                g_all(which).wait_send()
            if relay:
                r_all(which).wait_send()


def widen_kernel(blocks, density, residual, density_out, residual_out, narrow, wide, in_sem, out_sem):
    rows = density.shape[0] // blocks
    sources = (density, residual)
    targets = (density_out, residual_out)
    steps = [(w, pl.ds(n * rows, rows), n) for n in range(blocks) for w in range(2)]
    for w, part, n in steps:
        pltpu.make_async_copy(sources[w].at[part], narrow.at[w, part], in_sem.at[w, n]).start()
    for w, part, n in steps:
        pltpu.make_async_copy(sources[w].at[part], narrow.at[w, part], in_sem.at[w, n]).wait()
        wide[w, part] = narrow[w, part].astype(F32)
        pltpu.make_async_copy(wide.at[w, part], targets[w].at[part], out_sem.at[w, n]).start()
    for w, part, n in steps:
        pltpu.make_async_copy(wide.at[w, part], targets[w].at[part], out_sem.at[w, n]).wait()


def widen(density, residual):
    blocks = min(4, density.shape[0])
    hbm = pl.BlockSpec(memory_space=pl.ANY)
    field = jax.ShapeDtypeStruct(density.shape, F32)
    return pl.pallas_call(
        functools.partial(widen_kernel, blocks),
        in_specs=[hbm] * 2,
        out_specs=(hbm, hbm),
        out_shape=(field, field),
        scratch_shapes=[
            pltpu.VMEM((2,) + density.shape, BF),
            pltpu.VMEM((2,) + density.shape, F32),
            pltpu.SemaphoreType.DMA((2, blocks)),
            pltpu.SemaphoreType.DMA((2, blocks)),
        ],
        name="widen",
    )(density, residual)


def solution(mesh):
    G = mesh.shape["grid"]
    B = mesh.shape["band"]

    def local(
        bands,
        occupations,
        external,
        density_in,
        prev_density,
        prev_residual,
        hist_density,
        hist_residual,
    ):
        NB = bands.shape[1]
        S, NG = external.shape[0], external.shape[1]
        M = max(1, min(B, S // 8))
        H = B // M
        PL = S // M
        C = NG // 2 // G
        K = PL
        PB = PL // K
        GK = min(4, PL)
        dims = (G, M, H, NB, PL, C, K, PB, GK, NG)
        peers = G * M
        hbm = pl.BlockSpec(memory_space=pl.ANY)
        smem = pl.BlockSpec(memory_space=pltpu.SMEM)
        field = jax.ShapeDtypeStruct((S, NG, NG), BF)
        dma = pltpu.SemaphoreType.DMA
        loads = 3 + 2 * (DEPTH - 1)
        tables = make_tables(NG)
        bands_held = NB * M
        scratch = [pltpu.VMEM(table.shape, table.dtype) for table in tables] + [
            pltpu.VMEM((NB, M, PL, NG, 2 * NG), BF),
            pltpu.VMEM((NB, peers, PL, C, NG), BF),
            pltpu.VMEM((NB, peers, PL, C, NG), BF),
            pltpu.VMEM((K, peers, PB, NB, C, NG), BF),
            pltpu.VMEM((K, peers, PB, NB, C, NG), BF),
            pltpu.VMEM((PL, NG, 2 * NG), BF),
            pltpu.VMEM((NG * (C + 8), NG), F32),
            pltpu.VMEM((NG, C * NG), BF),
            pltpu.VMEM((NG, C * NG), BF),
            pltpu.VMEM((C * (NG + 8), NG), F32),
            pltpu.VMEM((NG, bands_held * NG), BF),
            pltpu.VMEM((bands_held * NG, NG), BF),
            pltpu.VMEM((M, PL, NG, NG), F32),
            pltpu.VMEM((S, NG, NG), F32),
            pltpu.VMEM((S, NG, NG), F32),
            pltpu.VMEM((DEPTH, PL, NG, NG), F32),
            pltpu.VMEM((DEPTH, PL, NG, NG), F32),
            pltpu.VMEM((ITERS, PL, NG, NG), F32),
            pltpu.VMEM((ITERS + 1, PL, NG, NG), F32),
            pltpu.VMEM((PL, NG, NG), F32),
            pltpu.VMEM((ITERS, H, PL, NG, NG), BF),
            pltpu.VMEM((ITERS, peers, 1, NG), F32),
            pltpu.VMEM((1 + DEPTH * (DEPTH + 1) // 2, 1, NG), F32),
            pltpu.VMEM((M, NB, 1, NG), F32),
            pltpu.VMEM((2, M, PL, NG, NG), BF),
            dma((len(tables),)),
            dma((2, M)),
            dma((NB, 2, M)),
            dma((loads,)),
            dma((NB,)),
            dma((NB,)),
            dma((K,)),
            dma((K,)),
            dma((K,)),
            dma((ITERS, K)),
            dma((1,)),
            dma((1,)),
            dma((1,)),
            dma((1,)),
            dma((2,)),
            dma((2, GK, M)),
            dma((2,)),
            dma((2,)),
            dma((2, M)),
        ]
        density, residual = pl.pallas_call(
            functools.partial(kernel, dims),
            in_specs=[smem] + [hbm] * (7 + len(tables)),
            out_specs=(hbm, hbm),
            out_shape=(field, field),
            scratch_shapes=scratch,
            compiler_params=pltpu.CompilerParams(
                collective_id=0, has_side_effects=True, vmem_limit_bytes=60 * 1024 * 1024
            ),
            name="scf",
        )(
            occupations,
            bands,
            external,
            density_in,
            prev_density,
            prev_residual,
            hist_density,
            hist_residual,
            *tables,
        )
        return widen(density, residual)

    placed = (
        P(None, "band", "grid", None, None),
        P("band"),
        P("grid", None, None),
        P("grid", None, None),
        P("grid", None, None),
        P("grid", None, None),
        P(None, "grid", None, None),
        P(None, "grid", None, None),
    )
    return jax.shard_map(
        local,
        mesh=mesh,
        in_specs=placed,
        out_specs=(P("grid", None, None), P("grid", None, None)),
        check_vma=False,
    )
```

```python
import contextlib
import functools
import math

import jax
import jax.numpy as jnp
import numpy as np
from jax import lax
from jax.experimental import pallas as pl
from jax.experimental.pallas import tpu as pltpu
from jax.sharding import PartitionSpec as P

DEPTH = 6
ITERS = 3

time_step = 0.25
energy_shift = 2.5
coupling = 1.0
mixing_weight = 0.5
ridge_share = 0.1
ridge_floor = 0.01
density_scale = 8.0

MESH = pl.DeviceIdType.MESH


def mark(name):
    return contextlib.nullcontext()

BF = jnp.bfloat16
F32 = jnp.float32


def make_tables(ng):
    freq = np.arange(-(ng // 4), ng // 4)
    phase = (np.arange(ng)[:, None] * freq[None, :]) % ng
    angles = phase.astype(np.float64) * (2.0 * math.pi / ng)
    cos = (np.cos(angles) / math.sqrt(ng)).astype(np.float32)
    sin = (np.sin(angles) / math.sqrt(ng)).astype(np.float32)
    forward_z = np.concatenate(
        [np.concatenate([cos, -sin, -sin, -cos], 1), np.concatenate([sin, cos, cos, -sin], 1)], 0
    )
    forward = np.concatenate([cos.T, sin.T], 1)
    forward_x = np.concatenate([cos.T, sin.T], 0)
    inverse = np.concatenate([cos, -sin], 1)
    inverse_z = np.concatenate(
        [np.concatenate([cos.T, sin.T], 1), np.concatenate([-sin.T, cos.T], 1)], 0
    )
    quarter = ng / 4.0
    damp = np.exp(-time_step * (freq.astype(np.float64) ** 2) / (quarter * quarter))
    damp = damp * ((freq >= -(ng // 4)) & (freq < ng // 4))
    pair = damp[:, None] * np.concatenate([damp, damp])[None, :]
    single = np.broadcast_to(damp[:, None], (damp.shape[0], 2 * damp.shape[0]))
    as_bf = lambda table: jnp.asarray(table, F32).astype(BF)
    return (
        as_bf(forward_z),
        as_bf(forward),
        as_bf(forward_x),
        as_bf(inverse),
        as_bf(inverse_z),
        jnp.asarray(pair, F32),
        jnp.asarray(np.ascontiguousarray(single), F32),
    )


def dot(a, b):
    return jnp.dot(a, b, preferred_element_type=F32)


def fold(cells):
    return jnp.sum(cells.reshape(-1, 8, cells.shape[-1]), axis=0)


def spot(j, k):
    return (j * (j + 1) // 2 + k) if j >= k else (k * (k + 1) // 2 + j)


def solve(gram, vector):
    trace = gram[0, 0]
    for j in range(1, DEPTH):
        trace = trace + gram[j, j]
    ridge = trace * (ridge_share / DEPTH) + ridge_floor
    matrix = {(j, k): gram[j, k] + ridge if j == k else gram[j, k] for (j, k) in gram}
    vector = list(vector)
    inverse = []
    for k in range(DEPTH):
        inverse.append(1.0 / matrix[k, k])
        scaled = {j: matrix[j, k] * inverse[k] for j in range(k + 1, DEPTH)}
        for j in range(k + 1, DEPTH):
            vector[j] = vector[j] - scaled[j] * vector[k]
            for m in range(k + 1, j + 1):
                matrix[j, m] = matrix[j, m] - scaled[j] * matrix[m, k]
    for k in reversed(range(DEPTH)):
        value = vector[k]
        for j in range(k + 1, DEPTH):
            value = value - matrix[j, k] * vector[j]
        vector[k] = value * inverse[k]
    return vector


def kernel(
    dims,
    occ_in,
    bands,
    external,
    density_in,
    prev_density,
    prev_residual,
    hist_density,
    hist_residual,
    fz_in,
    fy_in,
    fx_in,
    iy_in,
    iz_in,
    pair_in,
    single_in,
    density_out,
    residual_out,
    fz,
    fy,
    fx,
    iy,
    iz,
    pair_damp,
    single_damp,
    psi,
    send_f,
    recv_f,
    send_b,
    recv_b,
    along_z,
    xscr,
    xrhs,
    crhs,
    dscr,
    drhs,
    erows,
    fac,
    ext,
    rho0,
    q_hist,
    t_hist,
    now,
    res,
    prev,
    parts,
    sums,
    gsc,
    occ,
    gath,
    table_sem,
    field_sem,
    band_sem,
    load_sem,
    f_send,
    f_recv,
    b_send,
    b_recv,
    e_send,
    e_recv,
    a_send,
    a_recv,
    o_send,
    o_recv,
    g_send,
    g_recv,
    r_send,
    r_recv,
    out_sem,
):
    G, M, H, NB, PL, C, K, PB, GK, NG = dims
    GP = PL // GK
    relay = M == 4 and GP % 2 == 0
    kept = C * G
    peers = G * M
    xs = C + 8
    ds = NG + 8
    g = lax.axis_index("grid")
    b = lax.axis_index("band")
    m = lax.rem(b, M)
    h = b // M
    rank = m * G + g

    paired = M == 4 and G == 4

    def across(a, v):
        high, low, vh, vl = a // 2, lax.rem(a, 2), v // 2, v % 2
        return 2 * (high + vh - 2 * high * vh) + low + vl - 2 * low * vl

    def block_at(n):
        return across(m, M - 1 - n) if paired else lax.rem(m + 1 + n, M)

    def lane_at(r):
        return across(g, G - r) if paired else lax.rem(g + r, G)

    def place(r):
        if paired:
            v = peers - r
            return across(m, v // G), across(g, v % G)
        other = lax.rem(rank + r, peers)
        return other // G, lax.rem(other, G)

    def device(mm, gg):
        return (h * M + mm, gg)

    places = [None] + [place(r) for r in range(1, peers)]
    lanes = [None] + [lane_at(r) for r in range(1, G)] + [g]

    loads = []

    def load(src, dst):
        copy = pltpu.make_async_copy(src, dst, load_sem.at[len(loads)])
        loads.append(copy)
        return copy

    tables = [
        pltpu.make_async_copy(src, dst, table_sem.at[n])
        for n, (src, dst) in enumerate(
            (
                (fz_in, fz),
                (fy_in, fy),
                (fx_in, fx),
                (iy_in, iy),
                (iz_in, iz),
                (pair_in, pair_damp),
                (single_in, single_damp),
            )
        )
    ]

    def field_load(n, i):
        block = pl.ds(block_at(n) * PL, PL)
        src, dst = ((external, ext), (density_in, rho0))[i]
        return pltpu.make_async_copy(src.at[block], dst.at[block], field_sem.at[i, n])

    def band_load(t, n, c):
        j = block_at(n)
        return pltpu.make_async_copy(
            bands.at[c, t, pl.ds(j * PL, PL)],
            psi.at[t, j, :, :, pl.ds(c * NG, NG)],
            band_sem.at[t, c, n],
        )

    def start_block(n):
        field_load(n, 0).start()
        field_load(n, 1).start()
        band_load(0, n, 0).start()
        band_load(0, n, 1).start()

    for copy in tables:
        copy.start()
    for n in range(min(2, M)):
        start_block(n)
    mine = pl.ds(m * PL, PL)
    later = [
        load(density_in.at[mine], now.at[0]),
        load(prev_density.at[mine], prev),
        load(prev_residual.at[mine], res.at[0]),
    ]
    for j in range(DEPTH - 1):
        later.append(load(hist_residual.at[j, mine], q_hist.at[j]))
        later.append(load(hist_density.at[j, mine], t_hist.at[j]))

    barrier = pltpu.get_barrier_semaphore()

    def greet(r, _):
        mm, gg = place(r)
        pl.semaphore_signal(barrier, inc=1, device_id=device(mm, gg), device_id_type=MESH)
        return 0

    lax.fori_loop(1, peers, greet, 0)

    def greet_half(r, _):
        hh = lax.rem(h + r, H)
        pl.semaphore_signal(barrier, inc=1, device_id=(hh * M + m, g), device_id_type=MESH)
        return 0

    lax.fori_loop(1, H, greet_half, 0)

    lane = lax.broadcasted_iota(jnp.int32, (1, NG), 1)
    sign = jnp.where(lane < NG // 2, 1.0, -1.0).astype(F32)

    def rot(x):
        return pltpu.roll(x, NG // 2, 1) * sign

    lanes8 = lax.broadcasted_iota(jnp.int32, (8, NG), 1)

    def in_lanes(accs, offset):
        rows = jnp.zeros((8, NG), F32)
        for n, acc in enumerate(accs):
            rows = rows + jnp.where(lanes8 == offset + n, jnp.sum(acc, axis=1, keepdims=True), 0.0)
        return jnp.sum(rows, axis=0, keepdims=True)

    def f_copy(t, gg, j, slot, mm):
        return pltpu.make_async_remote_copy(
            src_ref=send_f.at[t, gg * M + j],
            dst_ref=recv_f.at[t, slot],
            send_sem=f_send.at[t],
            recv_sem=f_recv.at[t],
            device_id=device(mm, gg),
            device_id_type=MESH,
        )

    own = g * M + m

    def f_all(it, t):
        blocks = pl.ds(0, peers - M if it == 0 else peers - 1)
        mm, gg = places[1]
        return pltpu.make_async_remote_copy(
            src_ref=send_f.at[t, blocks],
            dst_ref=recv_f.at[t, blocks],
            send_sem=f_send.at[t],
            recv_sem=f_recv.at[t],
            device_id=device(mm, gg),
            device_id_type=MESH,
        )

    def b_copy(k, r):
        mm, gg = place(r)
        return pltpu.make_async_remote_copy(
            src_ref=send_b.at[k, gg * M + mm],
            dst_ref=recv_b.at[k, rank],
            send_sem=b_send.at[k],
            recv_sem=b_recv.at[k],
            device_id=device(mm, gg),
            device_id_type=MESH,
        )

    def b_all(k):
        mm, gg = places[1]
        return pltpu.make_async_remote_copy(
            src_ref=send_b.at[k, pl.ds(0, peers - 1)],
            dst_ref=recv_b.at[k, pl.ds(0, peers - 1)],
            send_sem=b_send.at[k],
            recv_sem=b_recv.at[k],
            device_id=device(mm, gg),
            device_id_type=MESH,
        )

    def e_copy(it, k, r):
        hh = lax.rem(h + r, H)
        rows = pl.ds(k * PB, PB)
        return pltpu.make_async_remote_copy(
            src_ref=parts.at[it, h, rows],
            dst_ref=parts.at[it, h, rows],
            send_sem=e_send.at[k],
            recv_sem=e_recv.at[it, k],
            device_id=(hh * M + m, g),
            device_id_type=MESH,
        )

    def e_all(it, k):
        hh = lax.rem(h + 1, H)
        part = parts.at[it, pl.ds(0, H - 1), pl.ds(k * PB, PB)]
        return pltpu.make_async_remote_copy(
            src_ref=part,
            dst_ref=part,
            send_sem=e_send.at[k],
            recv_sem=e_recv.at[it, k],
            device_id=(hh * M + m, g),
            device_id_type=MESH,
        )

    def a_copy(it, r):
        mm, gg = places[r]
        return pltpu.make_async_remote_copy(
            src_ref=sums.at[it, rank],
            dst_ref=sums.at[it, rank],
            send_sem=a_send.at[0],
            recv_sem=a_recv.at[0],
            device_id=device(mm, gg),
            device_id_type=MESH,
        )

    def a_all(it):
        mm, gg = places[1]
        part = sums.at[it, pl.ds(0, peers - 1)]
        return pltpu.make_async_remote_copy(
            src_ref=part,
            dst_ref=part,
            send_sem=a_send.at[0],
            recv_sem=a_recv.at[0],
            device_id=device(mm, gg),
            device_id_type=MESH,
        )

    def o_copy(r):
        mm = lax.rem(m + r, M)
        return pltpu.make_async_remote_copy(
            src_ref=occ.at[m],
            dst_ref=occ.at[m],
            send_sem=o_send.at[0],
            recv_sem=o_recv.at[0],
            device_id=device(mm, g),
            device_id_type=MESH,
        )

    def o_all():
        part = occ.at[pl.ds(0, M - 1)]
        return pltpu.make_async_remote_copy(
            src_ref=part,
            dst_ref=part,
            send_sem=o_send.at[0],
            recv_sem=o_recv.at[0],
            device_id=device(lax.rem(m + 1, M), g),
            device_id_type=MESH,
        )

    def near(r):
        if not relay:
            return lax.rem(m + r, M)
        return m + 1 - 2 * lax.rem(m, 2) if r == 1 else lax.rem(m + 2, M)

    direct = (1, 2) if relay else tuple(range(1, M))

    def g_copy(which, k, r):
        rows = pl.ds(k * GP, GP)
        return pltpu.make_async_remote_copy(
            src_ref=gath.at[which, m, rows],
            dst_ref=gath.at[which, m, rows],
            send_sem=g_send.at[which],
            recv_sem=g_recv.at[which, k, r - 1],
            device_id=device(near(r), g),
            device_id_type=MESH,
        )

    def r_copy(which, k, r):
        rows = pl.ds(k * GP + (r - 1) * (GP // 2), GP // 2)
        block = near(r)
        return pltpu.make_async_remote_copy(
            src_ref=gath.at[which, block, rows],
            dst_ref=gath.at[which, block, rows],
            send_sem=r_send.at[which],
            recv_sem=r_recv.at[which],
            device_id=device(near(3 - r), g),
            device_id_type=MESH,
        )

    def r_all(which):
        return pltpu.make_async_remote_copy(
            src_ref=gath.at[which, 0],
            dst_ref=gath.at[which, 0],
            send_sem=r_send.at[which],
            recv_sem=r_recv.at[which],
            device_id=device(near(1), g),
            device_id_type=MESH,
        )

    def g_all(which):
        part = gath.at[which, pl.ds(0, len(direct))]
        return pltpu.make_async_remote_copy(
            src_ref=part,
            dst_ref=part,
            send_sem=g_send.at[which],
            recv_sem=g_recv.at[which, 0, 0],
            device_id=device(near(1), g),
            device_id_type=MESH,
        )

    def g_start(which, k):
        for r in direct:
            g_copy(which, k, r).start()

    def g_pass_on(which, k):
        for r in direct:
            if relay:
                g_copy(which, k, r).wait_recv()
                r_copy(which, k, r).start()

    def start_all(make, count):
        for r in range(1, count):
            make(r).start()

    def start_paced(make, count):
        def body(r, _):
            make(r).start()
            return 0

        lax.fori_loop(1, count, body, 0)

    def forward_zy(it, t):
        def make(j):
            at = j if it == 0 else 0
            for q in range(PL):
                f = fac[at, q]
                real = (psi[t, j, q, :, :NG].astype(F32) * f).astype(BF)
                imag = (psi[t, j, q, :, NG:].astype(F32) * f).astype(BF)
                along_z[q] = dot(jnp.concatenate([real, imag], axis=1), fz[...]).astype(BF)
            for two in range(PL // 2):
                even, odd = along_z[2 * two], along_z[2 * two + 1]
                top = jnp.concatenate([even[:, :NG], odd[:, :NG]], axis=1)
                low = jnp.concatenate([even[:, NG:], odd[:, NG:]], axis=1)
                out = dot(fy[...], jnp.concatenate([top, low], axis=0)).astype(BF)
                for side in range(2):
                    for gg in range(G):
                        send_f[t, gg * M + j, 2 * two + side] = out[
                            gg * C : (gg + 1) * C, side * NG : (side + 1) * NG
                        ]

        def send(j, upper):
            for r in range(1, upper):
                gg = lanes[r]
                if it == 0:
                    f_copy(t, gg, j, g * M + j, m).start()
                else:
                    f_copy(t, gg, j, own, j).start()

        def step(n, _):
            j = block_at(n)
            if it == 0 and t == 0:

                @pl.when(n + 2 < M)
                def _():
                    start_block(n + 2)

                @pl.when(n > 0)
                def _():
                    for tt in range(1, NB):
                        band_load(tt, n - 1, 0).start()
                        band_load(tt, n - 1, 1).start()

            if it == 0:
                band_load(t, n, 0).wait()
                band_load(t, n, 1).wait()
            if it == 0 and t == 0:
                field_load(n, 0).wait()
                field_load(n, 1).wait()
                for q in range(PL):
                    plane = j * PL + q
                    fac[j, q] = jnp.exp(
                        -time_step * (ext[plane] + coupling * rho0[plane] - energy_shift)
                    )
            make(j)
            send(j, G if it == 0 else G + 1)
            if it == 0:
                recv_f[t, g * M + j] = send_f[t, g * M + j]
            return 0

        if it == 0:
            lax.fori_loop(0, M, step, 0)
            if t == 0:
                for tt in range(1, NB):
                    band_load(tt, M - 1, 0).start()
                    band_load(tt, M - 1, 1).start()
                for copy in later:
                    copy.start()
        else:
            lax.fori_loop(0, M - 1, step, 0)
            make(m)
            send(m, G)
            recv_f[t, own] = send_f[t, own]

    def spectral(t):
        def spread(blk, _):
            for p in range(PL):
                start = pl.multiple_of((blk * PL + p) * xs, 8)
                xscr[pl.ds(start, C), :] = recv_f[t, blk, p].astype(F32)
            return 0

        lax.fori_loop(0, peers, spread, 0)
        for kl in range(C):
            xrhs[:, kl * NG : (kl + 1) * NG] = xscr[pl.ds(kl, NG, stride=xs), :].astype(BF)
        for two in range(C // 2):
            c = dot(fx[...], xrhs[:, two * 2 * NG : (two + 1) * 2 * NG])
            for side in range(2):
                kl = 2 * two + side
                lanes = slice(side * NG, (side + 1) * NG)
                damp = pair_damp[...] * single_damp[pl.ds(g * C + kl, 1), :]
                one = (c[:kept, lanes] + rot(c[kept:, lanes])) * damp
                crhs[:kept, kl * NG : (kl + 1) * NG] = one.astype(BF)
                crhs[kept:, kl * NG : (kl + 1) * NG] = rot(one).astype(BF)
        for two in range(C // 2):
            d = dot(iy[...], crhs[:, two * 2 * NG : (two + 1) * 2 * NG])
            for side in range(2):
                kl = 2 * two + side
                dscr[kl * ds : kl * ds + NG, :] = d[:, side * NG : (side + 1) * NG]

    def collect(t, lowest, count):
        def body(blk, _):
            for p in range(lowest, lowest + count):
                v = dscr[pl.ds(blk * PL + p, C, stride=ds), :]
                send_b[p // PB, blk, p % PB, t] = v.astype(BF)
            return 0

        lax.fori_loop(0, peers, body, 0)

    def inverse_yz(it, k):
        def body(pp, _):
            p = k * PB + pp
            count = NB * M
            for n in range(count):
                d = jnp.concatenate(
                    [recv_b[k, n // NB * G + gg, pp, n % NB].astype(F32) for gg in range(G)], axis=0
                )
                drhs[:kept, n * NG : (n + 1) * NG] = d.astype(BF)
                drhs[kept:, n * NG : (n + 1) * NG] = rot(d).astype(BF)
            for two in range(count // 2):
                e = dot(iy[...], drhs[:, two * 2 * NG : (two + 1) * 2 * NG]).astype(BF)
                for side in range(2):
                    n = 2 * two + side
                    erows[n * NG : (n + 1) * NG, :] = e[:, side * NG : (side + 1) * NG]
            for n in range(count):
                psi[n % NB, n // NB, p] = dot(erows[n * NG : (n + 1) * NG, :], iz[...]).astype(BF)
            total = jnp.zeros((NG, NG), F32)
            for n in range(count):
                real = psi[n % NB, n // NB, p, :, :NG].astype(F32)
                imag = psi[n % NB, n // NB, p, :, NG:].astype(F32)
                total = total + occ[n // NB, n % NB] * (real * real + imag * imag)
            parts[it, h, p] = (total * (density_scale / (NB * M * H))).astype(BF)
            return 0

        lax.fori_loop(0, PB, body, 0)

    for t in range(NB):
        occ[m, t] = jnp.full((1, NG), occ_in[t], F32)

    for copy in tables:
        copy.wait()
    with mark("barrier"):
        pl.semaphore_wait(barrier, peers - 1 + H - 1)
    start_all(o_copy, M)

    cells = 1.0 / (NG * NG * NG)
    for it in range(ITERS):
        slot = (DEPTH - 1 + it) % DEPTH
        for t in range(NB):
            with mark(f"F{t}"):
                forward_zy(it, t)
        if it == 0:
            with mark("later"):
                for copy in later:
                    copy.wait()

            def prepare(p, accs):
                entries = [q_hist[j, p] for j in range(DEPTH - 1)]
                out = list(accs)
                for j in range(DEPTH - 1):
                    t_hist[j, p] = t_hist[j, p] + mixing_weight * entries[j]
                    for kk in range(j + 1):
                        out[spot(j, kk)] = out[spot(j, kk)] + fold(entries[j] * entries[kk])
                return tuple(out)

            zeros = tuple(jnp.zeros((8, NG), F32) for _ in range(spot(DEPTH - 1, 0)))
            with mark("prepare"):
                kept_sums = lax.fori_loop(0, PL, prepare, zeros)
            gsc[0] = in_lanes(kept_sums, 2 * DEPTH)
        for t in range(NB):
            with mark(f"waitF{t}"):
                f_all(it, t).wait_recv()
            with mark(f"X{t}"):
                spectral(t)
            with mark(f"collect{t}"):
                if t < NB - 1:
                    collect(t, 0, PL)
                else:
                    for k in range(K):
                        collect(t, k * PB, PB)
                        start_paced(functools.partial(b_copy, k), peers)
                        recv_b[k, rank] = send_b[k, own]
        if it == 0 and M > 1:
            o_all().wait_recv()
        for k in range(K):
            with mark(f"waitB{k}"):
                b_all(k).wait_recv()
            with mark(f"C{k}"):
                inverse_yz(it, k)
            start_all(functools.partial(e_copy, it, k), H)

        accs = tuple(jnp.zeros((8, NG), F32) for _ in range(2 * DEPTH))
        for k in range(K):
            with mark(f"waitE{k}"):
                if H > 1:
                    e_all(it, k).wait_recv()

            def gather_sums(p, accs, it=it, slot=slot):
                rho = parts[it, 0, p].astype(F32)
                for hh in range(1, H):
                    rho = rho + parts[it, hh, p].astype(F32)
                before = prev[p] if it == 0 else now[it - 1, p]
                here = now[it, p]
                residual = rho - here
                newest = residual - res[it, p]
                res[it + 1, p] = residual
                q_hist[slot, p] = newest
                t_hist[slot, p] = (here - before) + mixing_weight * newest
                out = list(accs)
                for j in range(DEPTH):
                    entry = newest if j == slot else q_hist[j, p]
                    out[j] = out[j] + fold(entry * newest)
                    out[DEPTH + j] = out[DEPTH + j] + fold(entry * residual)
                if it == ITERS - 1:
                    gath[1, m, p] = residual.astype(BF)
                return tuple(out)

            with mark(f"gram{k}"):
                accs = lax.fori_loop(k * PB, (k + 1) * PB, gather_sums, accs)
            ready = (k + 1) * PB
            if it == ITERS - 1 and ready % GP == 0 and ready < PL:
                g_start(1, ready // GP - 1)
        line = in_lanes(accs, 0)
        sums[it, rank] = gsc[0] + line if it == 0 else line
        start_all(functools.partial(a_copy, it), peers)
        if it == ITERS - 1:
            g_start(1, GK - 1)
            for k in range(GK - 2):
                g_pass_on(1, k)
        for t in range(NB):
            f_all(it, t).wait_send()
        for k in range(K):
            b_all(k).wait_send()
            if H > 1:
                e_all(it, k).wait_send()
        with mark("waitA"):
            a_all(it).wait_recv()
        total = sums[it, 0]
        for r in range(1, peers):
            total = total + sums[it, r]
        total = total * cells

        def pick(n):
            value = jnp.sum(jnp.where(lane == n, total, 0.0), axis=1, keepdims=True)
            return jnp.broadcast_to(value, (1, NG))

        if it == 0:
            for n in range(spot(DEPTH - 1, 0)):
                gsc[1 + n] = pick(2 * DEPTH + n)
        vector = [pick(DEPTH + j) for j in range(DEPTH)]
        for j in range(DEPTH):
            gsc[1 + spot(j, slot)] = pick(j)
        gram = {(j, kk): gsc[1 + spot(j, kk)] for j in range(DEPTH) for kk in range(j + 1)}
        with mark("solve"):
            coeffs = solve(gram, vector)

        def mix(p, _, it=it, coeffs=coeffs):
            value = now[it, p] + mixing_weight * res[it + 1, p]
            for j in range(DEPTH):
                value = value - coeffs[j] * t_hist[j, p]
            if it == ITERS - 1:
                gath[0, m, p] = value.astype(BF)
            else:
                now[it + 1, p] = value
                own = ext[m * PL + p]
                fac[0, p] = jnp.exp(-time_step * (own + coupling * value - energy_shift))
            return 0

        a_all(it).wait_send()
        with mark("mix"):
            for k in range(GK):
                lax.fori_loop(k * GP, (k + 1) * GP, mix, 0)
                if it == ITERS - 1:
                    g_start(0, k)

    def out_copy(which, block):
        out = density_out if which == 0 else residual_out
        return pltpu.make_async_copy(
            gath.at[which, block], out.at[pl.ds(block * PL, PL)], out_sem.at[which, block]
        )

    with mark("pass"):
        for k in range(max(GK - 2, 0), GK):
            g_pass_on(1, k)
        for k in range(GK):
            g_pass_on(0, k)
    for which in (1, 0):
        out_copy(which, m).start()
        for r in direct:
            if not relay:
                for k in range(GK):
                    g_copy(which, k, r).wait_recv()
            out_copy(which, near(r)).start()
        if relay:
            with mark(f"waitR{which}"):
                r_all(which).wait_recv()
            out_copy(which, 3 - m).start()
    with mark("outs"):
        for which in (1, 0):
            for block in range(M):
                out_copy(which, block).wait()
    with mark("drain"):
        if M > 1:
            o_all().wait_send()
        for which in range(2):
            if direct:
                g_all(which).wait_send()
            if relay:
                r_all(which).wait_send()


def widen_kernel(blocks, density, residual, density_out, residual_out, narrow, wide, in_sem, out_sem):
    rows = density.shape[0] // blocks
    sources = (density, residual)
    targets = (density_out, residual_out)
    steps = [(w, pl.ds(n * rows, rows), n) for n in range(blocks) for w in range(2)]
    for w, part, n in steps:
        pltpu.make_async_copy(sources[w].at[part], narrow.at[w, part], in_sem.at[w, n]).start()
    for w, part, n in steps:
        pltpu.make_async_copy(sources[w].at[part], narrow.at[w, part], in_sem.at[w, n]).wait()
        wide[w, part] = narrow[w, part].astype(F32)
        pltpu.make_async_copy(wide.at[w, part], targets[w].at[part], out_sem.at[w, n]).start()
    for w, part, n in steps:
        pltpu.make_async_copy(wide.at[w, part], targets[w].at[part], out_sem.at[w, n]).wait()


def widen(density, residual):
    blocks = min(4, density.shape[0])
    hbm = pl.BlockSpec(memory_space=pl.ANY)
    field = jax.ShapeDtypeStruct(density.shape, F32)
    return pl.pallas_call(
        functools.partial(widen_kernel, blocks),
        in_specs=[hbm] * 2,
        out_specs=(hbm, hbm),
        out_shape=(field, field),
        scratch_shapes=[
            pltpu.VMEM((2,) + density.shape, BF),
            pltpu.VMEM((2,) + density.shape, F32),
            pltpu.SemaphoreType.DMA((2, blocks)),
            pltpu.SemaphoreType.DMA((2, blocks)),
        ],
        name="widen",
    )(density, residual)


def solution(mesh):
    G = mesh.shape["grid"]
    B = mesh.shape["band"]

    def local(
        bands,
        occupations,
        external,
        density_in,
        prev_density,
        prev_residual,
        hist_density,
        hist_residual,
    ):
        NB = bands.shape[1]
        S, NG = external.shape[0], external.shape[1]
        M = max(1, min(B, S // 8))
        H = B // M
        PL = S // M
        C = NG // 2 // G
        K = PL
        PB = PL // K
        GK = min(4, PL)
        dims = (G, M, H, NB, PL, C, K, PB, GK, NG)
        peers = G * M
        hbm = pl.BlockSpec(memory_space=pl.ANY)
        smem = pl.BlockSpec(memory_space=pltpu.SMEM)
        field = jax.ShapeDtypeStruct((S, NG, NG), BF)
        dma = pltpu.SemaphoreType.DMA
        loads = 3 + 2 * (DEPTH - 1)
        tables = make_tables(NG)
        bands_held = NB * M
        scratch = [pltpu.VMEM(table.shape, table.dtype) for table in tables] + [
            pltpu.VMEM((NB, M, PL, NG, 2 * NG), BF),
            pltpu.VMEM((NB, peers, PL, C, NG), BF),
            pltpu.VMEM((NB, peers, PL, C, NG), BF),
            pltpu.VMEM((K, peers, PB, NB, C, NG), BF),
            pltpu.VMEM((K, peers, PB, NB, C, NG), BF),
            pltpu.VMEM((PL, NG, 2 * NG), BF),
            pltpu.VMEM((NG * (C + 8), NG), F32),
            pltpu.VMEM((NG, C * NG), BF),
            pltpu.VMEM((NG, C * NG), BF),
            pltpu.VMEM((C * (NG + 8), NG), F32),
            pltpu.VMEM((NG, bands_held * NG), BF),
            pltpu.VMEM((bands_held * NG, NG), BF),
            pltpu.VMEM((M, PL, NG, NG), F32),
            pltpu.VMEM((S, NG, NG), F32),
            pltpu.VMEM((S, NG, NG), F32),
            pltpu.VMEM((DEPTH, PL, NG, NG), F32),
            pltpu.VMEM((DEPTH, PL, NG, NG), F32),
            pltpu.VMEM((ITERS, PL, NG, NG), F32),
            pltpu.VMEM((ITERS + 1, PL, NG, NG), F32),
            pltpu.VMEM((PL, NG, NG), F32),
            pltpu.VMEM((ITERS, H, PL, NG, NG), BF),
            pltpu.VMEM((ITERS, peers, 1, NG), F32),
            pltpu.VMEM((1 + DEPTH * (DEPTH + 1) // 2, 1, NG), F32),
            pltpu.VMEM((M, NB, 1, NG), F32),
            pltpu.VMEM((2, M, PL, NG, NG), BF),
            dma((len(tables),)),
            dma((2, M)),
            dma((NB, 2, M)),
            dma((loads,)),
            dma((NB,)),
            dma((NB,)),
            dma((K,)),
            dma((K,)),
            dma((K,)),
            dma((ITERS, K)),
            dma((1,)),
            dma((1,)),
            dma((1,)),
            dma((1,)),
            dma((2,)),
            dma((2, GK, 2 if M == 4 else max(1, M - 1))),
            dma((2,)),
            dma((2,)),
            dma((2, M)),
        ]
        density, residual = pl.pallas_call(
            functools.partial(kernel, dims),
            in_specs=[smem] + [hbm] * (7 + len(tables)),
            out_specs=(hbm, hbm),
            out_shape=(field, field),
            scratch_shapes=scratch,
            compiler_params=pltpu.CompilerParams(
                collective_id=0, has_side_effects=True, vmem_limit_bytes=60 * 1024 * 1024
            ),
            name="scf",
        )(
            occupations,
            bands,
            external,
            density_in,
            prev_density,
            prev_residual,
            hist_density,
            hist_residual,
            *tables,
        )
        return widen(density, residual)

    placed = (
        P(None, "band", "grid", None, None),
        P("band"),
        P("grid", None, None),
        P("grid", None, None),
        P("grid", None, None),
        P("grid", None, None),
        P(None, "grid", None, None),
        P(None, "grid", None, None),
    )
    return jax.shard_map(
        local,
        mesh=mesh,
        in_specs=placed,
        out_specs=(P("grid", None, None), P("grid", None, None)),
        check_vma=False,
    )
```
